256 devices in a mesh: site: 2 (over y_lo), rows: 16 (over z, core), width: 8 (over y_hi, x).
Axes of the slice: x: 4, y: 4 (y_hi: 2, y_lo: 2; y = y_hi * 2 + y_lo), z: 8, core: 2. Of those that a mesh axis runs over, the one named last changes fastest.
Arguments:
- one_query: float32 [14336, 7168], P(('site', 'rows'), 'width'), parts along dimension 0, may hold values from -0.09375 to 0.09375
- other_query: float32 [14336, 7168], P(('site', 'rows'), 'width'), parts along dimension 0, may hold values from -0.0625 to 0.0625
- one_key: float32 [14336, 1024], P(('site', 'rows'), 'width'), parts along dimension 0, may hold values from -0.09375 to 0.09375
- other_key: float32 [14336, 1024], P(('site', 'rows'), 'width'), parts along dimension 0, may hold values from -0.0625 to 0.0625
- one_value: float32 [14336, 1024], P(('site', 'rows'), 'width'), parts along dimension 0, may hold values from -0.09375 to 0.09375
- other_value: float32 [14336, 1024], P(('site', 'rows'), 'width'), parts along dimension 0, may hold values from -0.0625 to 0.0625
- mix_share: float32 [14336], P(('site', 'rows')), parts along dimension 0, may hold values from 0.2 to 0.8
- norm_train: float32 [14336], P(('site', 'rows', 'width')), parts along dimension 0, may hold values from 0.25 to 1.75
- norm_step: float32 [14336], P(('site', 'rows', 'width')), parts along dimension 0, may hold values from -0.3 to 0.3
Outputs:
- serving_query: bfloat16 [14336, 7168], P('site', 'width'), parts along dimension 0
- serving_key: bfloat16 [14336, 1024], P('site', 'width'), parts along dimension 0
- serving_value: bfloat16 [14336, 1024], P('site', 'width'), parts along dimension 0
- scale_query: float32 [14336], P(('site', 'width')), parts along dimension 0
- scale_key: float32 [2048], P(('site', 'width')), parts along dimension 0
- scale_value: float32 [2048], P(('site', 'width')), parts along dimension 0
- serve_norm: bfloat16 [14336], P('site'), parts along dimension 0
The draws below stay inside these ranges and needn't reach their ends.
There are 2 independent parts, one for each index of `site`. The reference program is written for one: setup_inputs(seed, part) draws one part's arguments, and reference() takes and returns one part's arrays. A program takes and returns all parts, laid end to end along the dimension named above; each array names one. Nothing has to cross between parts.
All inputs are finite; a program needn't handle non-finite values. Where the reference program divides by a largest or mean magnitude, that divisor is 1e-20 or more.
Results may differ from the reference program's by a relative error of at most 0.001.
Values may be sent and summed in bfloat16 or wider, within the bound.
A program may use at most 128 MiB of HBM per device.

```python
import jax
import jax.numpy as jnp

D_MODEL = 7168
Q_DIM = 7168
KV_DIM = 1024


def raised(drawn, rng, source, target, blocks, factor):
    def block_of(dim):
        return (jnp.arange(drawn.shape[dim]) // (drawn.shape[dim] // blocks)).reshape((-1,) + (1,) * (drawn.ndim - 1 - dim))

    first = jax.random.permutation(rng, blocks)[block_of(target)]
    other_side = (block_of(target) + blocks // 2) % blocks
    return jnp.where((block_of(source) == first) | (block_of(source) == other_side), factor * drawn, drawn)


def level_of(own_key, dims, cuts, least, largest):
    loudness = 1.0
    for position, blocks in cuts:
        heights = jax.random.uniform(jax.random.fold_in(jax.random.fold_in(own_key, 6), position), (blocks,), jnp.float32, least / len(cuts), largest / len(cuts))
        loudness = loudness * jnp.repeat(jnp.exp(heights), dims[position] // blocks).reshape((-1,) + (1,) * (len(dims) - 1 - position))
    return loudness


def gaussian(stream_key, shape, width, most, shards=(), kind=jnp.bfloat16):
    result = jax.random.normal(stream_key, shape, jnp.float32) * width
    if len(shards) > 0:
        result = level_of(stream_key, shape, shards, -0.22, 0.18) * result
    return jnp.clip(result, min=-most, max=most).astype(kind)


def bell_draw_with(stream_key, extent, spread, reach, cuts, heavy, dtype=jnp.bfloat16):
    result = spread * jax.random.normal(stream_key, extent, jnp.float32)
    if cuts:
        result = result * level_of(stream_key, extent, cuts, -0.22, 0.18)
    return jnp.clip(raised(result, jax.random.fold_in(stream_key, 3), *heavy), -reach, reach).astype(dtype)


def setup_inputs(seed: int = 0, part: int = 0) -> dict:
    seeds = jax.random.split(jax.random.key(seed), 10)
    part_splits = jax.random.split(jax.random.fold_in(seeds[9], part), 10)
    return {
        "one_query": bell_draw_with(part_splits[0], (D_MODEL, Q_DIM), D_MODEL ** -0.5, 0.09375, ((0, 16), (1, 8)), (0, 1, 16, 2.0), jnp.float32),
        "other_query": gaussian(part_splits[1], (D_MODEL, Q_DIM), D_MODEL ** -0.5, 0.0625, ((0, 16), (1, 8)), jnp.float32),
        "one_key": bell_draw_with(part_splits[2], (D_MODEL, KV_DIM), D_MODEL ** -0.5, 0.09375, ((0, 16), (1, 8)), (0, 1, 16, 2.0), jnp.float32),
        "other_key": gaussian(part_splits[3], (D_MODEL, KV_DIM), D_MODEL ** -0.5, 0.0625, ((0, 16), (1, 8)), jnp.float32),
        "one_value": bell_draw_with(part_splits[4], (D_MODEL, KV_DIM), D_MODEL ** -0.5, 0.09375, ((0, 16), (1, 8)), (0, 1, 16, 2.0), jnp.float32),
        "other_value": gaussian(part_splits[5], (D_MODEL, KV_DIM), D_MODEL ** -0.5, 0.0625, ((0, 16), (1, 8)), jnp.float32),
        "mix_share": jnp.clip(0.2 + 0.6 * jax.random.uniform(part_splits[6], (D_MODEL,), jnp.float32) ** level_of(part_splits[6], (D_MODEL,), ((0, 16),), -0.2, 0.2), 0.2, 0.8),
        "norm_train": jnp.clip(1.0 + 0.15 * jax.random.normal(part_splits[7], (D_MODEL,), jnp.float32), 0.25, 1.75),
        "norm_step": jnp.clip(jax.random.uniform(part_splits[8], (D_MODEL,), jnp.float32, -0.3, 0.3) * level_of(part_splits[8], (D_MODEL,), ((0, 128),), -0.4, 0.0), -0.3, 0.3),
    }


def reference(one_query, other_query, one_key, other_key, one_value, other_value, mix_share, norm_train, norm_step):
    whole_query = mix_share[:, None] * one_query + (1.0 - mix_share[:, None]) * other_query
    whole_key = mix_share[:, None] * one_key + (1.0 - mix_share[:, None]) * other_key
    whole_value = mix_share[:, None] * one_value + (1.0 - mix_share[:, None]) * other_value
    scale_query = jnp.max(jnp.abs(whole_query), axis=0)
    serving_query = (whole_query / scale_query).astype(jnp.bfloat16)
    scale_key = jnp.max(jnp.abs(whole_key), axis=0)
    serving_key = (whole_key / scale_key).astype(jnp.bfloat16)
    scale_value = jnp.max(jnp.abs(whole_value), axis=0)
    serving_value = (whole_value / scale_value).astype(jnp.bfloat16)
    serve_norm = (norm_train + norm_step).astype(jnp.bfloat16)
    return serving_query, serving_key, serving_value, scale_query, scale_key, scale_value, serve_norm
```

```python
import functools

import jax
import jax.numpy as jnp
from jax import lax
from jax.experimental import pallas as pl
from jax.experimental.pallas import tpu as pltpu
from jax.sharding import PartitionSpec as P

MESH = pl.DeviceIdType.MESH
LANES = 128
LOAD = 64


def bounds_of(rows):
    half = rows // 2
    cuts = [0, half // 2, half, half + half // 2, rows]
    return list(zip(cuts, cuts[1:]))


def gather_kernel(nrows, nwidth, dims, *refs):
    (one_q, other_q, one_k, other_k, one_v, other_v, mix_hbm, norm_t_hbm, norm_s_hbm,
     out, scale_q, scale_k, scale_v, norm_out,
     mix, norm_t, norm_s, a_buf, b_buf, mixb, acc, maxima, seg, tiles_w, tiles_r, joined,
     lead_sem, in_sem, max_send, max_recv, nw_send, nw_recv, nr_send, nr_recv,
     ring_send, ring_recv, share_send, share_recv) = refs
    rows, qd, kd = dims
    cols = qd + 2 * kd
    nz = nrows // 2
    r = lax.axis_index("rows")
    w = lax.axis_index("width")
    z, c = r // 2, lax.rem(r, 2)
    bounds = bounds_of(rows)
    nchunk = len(bounds)

    def row_peer(i):
        return {"rows": lax.rem(r + i, nrows)}

    def width_peer(i):
        return {"width": lax.rem(w + i, nwidth)}

    barrier = pltpu.get_barrier_semaphore()
    for i in range(1, nrows):
        pl.semaphore_signal(barrier, inc=1, device_id=row_peer(i), device_id_type=MESH)
    for i in range(1, nwidth):
        pl.semaphore_signal(barrier, inc=1, device_id=width_peer(i), device_id_type=MESH)

    leads = [
        pltpu.make_async_copy(src, dst, lead_sem.at[i])
        for i, (src, dst) in enumerate(((mix_hbm, mix), (norm_t_hbm, norm_t), (norm_s_hbm, norm_s)))
    ]
    for copy in leads:
        copy.start()
    parts = (
        (one_q, a_buf, 0, qd), (other_q, b_buf, 0, qd),
        (one_k, a_buf, qd, kd), (other_k, b_buf, qd, kd),
        (one_v, a_buf, qd + kd, kd), (other_v, b_buf, qd + kd, kd),
    )

    def loads(step):
        span = pl.ds(step * LOAD, LOAD)
        return [
            pltpu.make_async_copy(src.at[span, :], dst.at[span, pl.ds(at, n)], in_sem.at[step, i])
            for i, (src, dst, at, n) in enumerate(parts)
        ]

    for step in range(rows // LOAD):
        for copy in loads(step):
            copy.start()

    for copy in leads:
        copy.wait()

    for at in range(0, rows, LANES):
        n = min(LANES, rows - at)
        line = mix[:, at:at + n]
        if n < LANES:
            line = jnp.concatenate([line, jnp.zeros((1, LANES - n), jnp.float32)], axis=1)
        square = jnp.transpose(jnp.broadcast_to(line, (LANES, LANES)))
        mixb[at:at + n, :] = square[:n, :]

    small = norm_t.shape[1]
    pos = lax.rem(r, 2) * nwidth + w
    first, lane0 = (pos * small) // LANES, lax.rem(pos * small, LANES)
    seg[...] = jnp.zeros((8, LANES), jnp.float32)
    seg[0:1, 0:small] = norm_t[...] + norm_s[...]
    turned = pltpu.roll(seg[...], lane0, 1)[0:1, :]
    lane = lax.broadcasted_iota(jnp.int32, (8, LANES), 1)
    line = lax.broadcasted_iota(jnp.int32, (8, LANES), 0)
    here = ((line == first) & (lane >= lane0)) | ((line == first + 1) & (lane < lane0))
    tiles_w[w] = jnp.where(here, jnp.broadcast_to(turned, (8, LANES)), 0.0)

    acc[...] = jnp.zeros((8, cols), jnp.float32)
    for step in range(rows // LOAD):
        for copy in loads(step):
            copy.wait()
        span = slice(step * LOAD, (step + 1) * LOAD)
        m = mixb[span, :]
        rest = 1.0 - m
        for at in range(0, cols, LANES):
            lanes = slice(at, at + LANES)
            whole = m * a_buf[span, lanes] + rest * b_buf[span, lanes]
            a_buf[span, lanes] = whole
            top = jnp.max(jnp.abs(whole).reshape(LOAD // 8, 8, LANES), axis=0)
            acc[:, lanes] = jnp.maximum(acc[:, lanes], top)
    maxima[r] = jnp.max(acc[...], axis=0, keepdims=True)

    pl.semaphore_wait(barrier, nrows - 1 + nwidth - 1)

    order = sorted(range(1, nrows), key=lambda i: -min(i, nrows - i))

    def max_copy(i):
        return pltpu.make_async_remote_copy(
            src_ref=maxima.at[r], dst_ref=maxima.at[r], send_sem=max_send.at[i], recv_sem=max_recv.at[i],
            device_id=row_peer(i), device_id_type=MESH)

    def norm_w_copy(i):
        return pltpu.make_async_remote_copy(
            src_ref=tiles_w.at[w], dst_ref=tiles_w.at[w], send_sem=nw_send.at[i], recv_sem=nw_recv.at[i],
            device_id=width_peer(i), device_id_type=MESH)

    def norm_r_copy(i):
        return pltpu.make_async_remote_copy(
            src_ref=tiles_r.at[r], dst_ref=tiles_r.at[r], send_sem=nr_send.at[i], recv_sem=nr_recv.at[i],
            device_id=row_peer(i), device_id_type=MESH)

    for i in order:
        max_copy(i).start()
    for i in range(1, nwidth):
        norm_w_copy(i).start()
    for i in order:
        max_copy(i).wait_recv()
    scale = maxima[0]
    for i in range(1, nrows):
        scale = jnp.maximum(scale, maxima[i])
    for line in range(qd // LANES):
        scale_q[line:line + 1, :] = scale[:, line * LANES:(line + 1) * LANES]
    scale_k[...] = scale[:, qd:qd + kd]
    scale_v[...] = scale[:, qd + kd:]

    steps = (1, nrows - 1), (nz // 2, nz // 2)
    ahead = ({"rows": lax.rem(r + 2, nrows)}, {"rows": lax.rem(r + nrows - 2, nrows)})
    partner = {"rows": r + 1 - 2 * c}

    def block(direction, hop, chunk):
        lo, hi = bounds[chunk]
        owner = lax.rem(z - hop + nz, nz) if direction == 0 else lax.rem(z + hop, nz)
        at = (owner * 2 + c) * rows + lo
        return out.at[pl.ds(pl.multiple_of(at, 16), hi - lo), :]

    def ring(direction, hop, chunk):
        ref = block(direction, hop, chunk)
        return pltpu.make_async_remote_copy(
            src_ref=ref, dst_ref=ref, send_sem=ring_send.at[direction, hop, chunk],
            recv_sem=ring_recv.at[direction, hop, chunk], device_id=ahead[direction], device_id_type=MESH)

    def arrived(direction, hop, chunk):
        ref = block(direction, hop, chunk)
        return pltpu.make_async_remote_copy(
            src_ref=ref, dst_ref=ref, send_sem=ring_send.at[direction, hop - 1, chunk],
            recv_sem=ring_recv.at[direction, hop - 1, chunk], device_id=ahead[direction], device_id_type=MESH)

    def share(direction, hop, chunk):
        ref = block(direction, hop, chunk)
        return pltpu.make_async_remote_copy(
            src_ref=ref, dst_ref=ref, send_sem=share_send.at[direction, hop, chunk],
            recv_sem=share_recv.at[direction, hop, chunk], device_id=partner, device_id_type=MESH)

    far = nz // 2

    def chunks(direction, hop):
        if hop < far:
            return list(range(nchunk))
        return list(range(nchunk // 2)) if direction == 0 else list(range(nchunk // 2, nchunk))

    mine = r * rows
    for chunk, (lo, hi) in enumerate(bounds):
        for at in range(0, cols, LANES):
            lanes = slice(at, at + LANES)
            out[pl.ds(pl.multiple_of(mine + lo, 16), hi - lo), lanes] = (
                a_buf[lo:hi, lanes] / scale[:, lanes]).astype(out.dtype)
        ring(0, 0, chunk).start()
        ring(1, 0, chunk).start()
        share(0, 0, chunk).start()

    for i in range(1, nwidth):
        norm_w_copy(i).wait_recv()
    total = tiles_w[0]
    for i in range(1, nwidth):
        total = total + tiles_w[i]
    tiles_r[r] = total
    for i in order:
        norm_r_copy(i).start()

    for hop in range(1, far + 1):
        for pair in zip(*(chunks(d, hop) for d in (0, 1))):
            for direction, chunk in enumerate(pair):
                arrived(direction, hop, chunk).wait_recv()
                if hop + 1 <= far and chunk in chunks(direction, hop + 1):
                    ring(direction, hop, chunk).start()
                share(direction, hop, chunk).start()
        if hop == 1:
            for i in order:
                norm_r_copy(i).wait_recv()
            per = 2 * nwidth * small // LANES
            for g in range(nrows // 2):
                full = tiles_r[2 * g] + tiles_r[2 * g + 1]
                joined[g * per:(g + 1) * per, :] = full[:per, :]
            norm_out[...] = joined[...].astype(norm_out.dtype)

    for hop in range(far + 1):
        for direction in (0, 1) if hop else (0,):
            for chunk in chunks(direction, hop):
                lo, hi = bounds[chunk]
                owner = lax.rem(z - hop + nz, nz) if direction == 0 else lax.rem(z + hop, nz)
                at = (owner * 2 + 1 - c) * rows + lo
                ref = out.at[pl.ds(pl.multiple_of(at, 16), hi - lo), :]
                pltpu.make_async_remote_copy(
                    src_ref=ref, dst_ref=ref, send_sem=share_send.at[direction, hop, chunk],
                    recv_sem=share_recv.at[direction, hop, chunk], device_id=partner,
                    device_id_type=MESH).wait_recv()
                share(direction, hop, chunk).wait_send()
    for hop in range(far):
        for direction in (0, 1):
            for chunk in chunks(direction, hop + 1):
                ring(direction, hop, chunk).wait_send()
    for i in range(1, nrows):
        max_copy(i).wait_send()
        norm_r_copy(i).wait_send()
    for i in range(1, nwidth):
        norm_w_copy(i).wait_send()


def write_kernel(dims, full, *refs):
    qd, kd = dims
    q, k, v = refs[4:7]
    sems = refs[-1]
    rows = full.shape[0]
    pieces = 8
    step = rows // pieces
    copies = []
    for i in range(pieces):
        span = pl.ds(i * step, step)
        copies.append((full.at[span, pl.ds(0, qd)], q.at[span, :]))
        copies.append((full.at[span, pl.ds(qd, kd)], k.at[span, :]))
        copies.append((full.at[span, pl.ds(qd + kd, kd)], v.at[span, :]))
    copies.extend(zip(refs[:4], refs[7:11]))
    started = [pltpu.make_async_copy(src, dst, sems.at[i]) for i, (src, dst) in enumerate(copies)]
    for copy in started:
        copy.start()
    for copy in started:
        copy.wait()


def shards(nrows, nwidth, one_q, other_q, one_k, other_k, one_v, other_v, mix, norm_t, norm_s):
    rows, qd = one_q.shape
    kd = one_k.shape[1]
    cols = qd + 2 * kd
    small = norm_t.shape[0]
    total = rows * nrows
    lines = small * nrows * nwidth // LANES
    nz, nchunk = nrows // 2, len(bounds_of(rows))
    far = nz // 2
    hbm = pl.BlockSpec(memory_space=pltpu.HBM)
    vmem = pl.BlockSpec(memory_space=pltpu.VMEM)
    full, scale_q, scale_k, scale_v, norm = pl.pallas_call(
        functools.partial(gather_kernel, nrows, nwidth, (rows, qd, kd)),
        out_shape=(
            pltpu.VMEM((total, cols), jnp.bfloat16),
            pltpu.VMEM((qd // LANES, LANES), jnp.float32),
            pltpu.VMEM((1, kd), jnp.float32),
            pltpu.VMEM((1, kd), jnp.float32),
            pltpu.VMEM((lines, LANES), jnp.bfloat16),
        ),
        in_specs=[hbm] * 9,
        out_specs=(vmem,) * 5,
        scratch_shapes=[
            pltpu.VMEM((1, rows), jnp.float32),
            pltpu.VMEM((1, small), jnp.float32),
            pltpu.VMEM((1, small), jnp.float32),
            pltpu.VMEM((rows, cols), jnp.float32),
            pltpu.VMEM((rows, cols), jnp.float32),
            pltpu.VMEM((rows, LANES), jnp.float32),
            pltpu.VMEM((8, cols), jnp.float32),
            pltpu.VMEM((nrows, 1, cols), jnp.float32),
            pltpu.VMEM((8, LANES), jnp.float32),
            pltpu.VMEM((nwidth, 8, LANES), jnp.float32),
            pltpu.VMEM((nrows, 8, LANES), jnp.float32),
            pltpu.VMEM((lines, LANES), jnp.float32),
            pltpu.SemaphoreType.DMA((3,)),
            pltpu.SemaphoreType.DMA((rows // LOAD, 6)),
            pltpu.SemaphoreType.DMA((nrows,)),
            pltpu.SemaphoreType.DMA((nrows,)),
            pltpu.SemaphoreType.DMA((nwidth,)),
            pltpu.SemaphoreType.DMA((nwidth,)),
            pltpu.SemaphoreType.DMA((nrows,)),
            pltpu.SemaphoreType.DMA((nrows,)),
            pltpu.SemaphoreType.DMA((2, far, nchunk)),
            pltpu.SemaphoreType.DMA((2, far, nchunk)),
            pltpu.SemaphoreType.DMA((2, far + 1, nchunk)),
            pltpu.SemaphoreType.DMA((2, far + 1, nchunk)),
        ],
        compiler_params=pltpu.CompilerParams(
            collective_id=0, has_side_effects=True, vmem_limit_bytes=24 * 1024 * 1024),
        name="gather",
    )(*(pltpu.with_memory_space_constraint(x, pltpu.HBM) for x in (
        one_q, other_q, one_k, other_k, one_v, other_v,
        mix.reshape(1, -1), norm_t.reshape(1, -1), norm_s.reshape(1, -1))))
    q, k, v, scale_q, scale_k, scale_v, norm_o = pl.pallas_call(
        functools.partial(write_kernel, (qd, kd)),
        out_shape=(
            jax.ShapeDtypeStruct((total, qd), jnp.bfloat16),
            jax.ShapeDtypeStruct((total, kd), jnp.bfloat16),
            jax.ShapeDtypeStruct((total, kd), jnp.bfloat16),
            jax.ShapeDtypeStruct((qd // LANES, LANES), jnp.float32),
            jax.ShapeDtypeStruct((1, kd), jnp.float32),
            jax.ShapeDtypeStruct((1, kd), jnp.float32),
            jax.ShapeDtypeStruct((lines, LANES), jnp.bfloat16),
        ),
        in_specs=[vmem] * 5,
        out_specs=(hbm,) * 7,
        scratch_shapes=[pltpu.SemaphoreType.DMA((28,))],
        compiler_params=pltpu.CompilerParams(vmem_limit_bytes=1024 * 1024),
        name="write",
    )(full, scale_q, scale_k, scale_v, norm)
    return (q, k, v, scale_q.reshape(-1), scale_k.reshape(-1), scale_v.reshape(-1),
            norm_o.reshape(-1))


def solution(mesh):
    rows = ("site", "rows")
    return jax.shard_map(
        functools.partial(shards, mesh.shape["rows"], mesh.shape["width"]),
        mesh=mesh,
        in_specs=(P(rows, "width"),) * 6 + (P(rows), P(("site", "rows", "width")), P(("site", "rows", "width"))),
        out_specs=(P("site", "width"),) * 3 + (P(("site", "width")),) * 3 + (P("site"),),
        check_vma=False,
    )
```

```python
import functools

import jax
import jax.numpy as jnp
from jax import lax
from jax.experimental import pallas as pl
from jax.experimental.pallas import tpu as pltpu
from jax.sharding import PartitionSpec as P

MESH = pl.DeviceIdType.MESH
LANES = 128
LOAD = 56
ROOT = 1


def bounds_of(rows):
    half = rows // 2
    cuts = [0, half // 2, half - 32, half]
    cuts += [half + at for at in cuts[1:]]
    return list(zip(cuts, cuts[1:]))


def gather_kernel(nrows, nwidth, dims, *refs):
    (one_q, other_q, one_k, other_k, one_v, other_v, mix_hbm, norm_t_hbm, norm_s_hbm,
     out, scale_q, scale_k, scale_v, norm_out,
     mix, norm_t, norm_s, a_buf, b_buf, early, mixb, acc, maxima, seg, tiles, gains, joined,
     tokens, lead_sem, in_sem, max_send, max_recv, tile_send, tile_recv, gain_send, gain_recv, norm_send, norm_recv,
     early_send, early_recv, ring_send, ring_recv, share_send, share_recv) = refs
    rows, qd, kd = dims
    cols = qd + 2 * kd
    nz = nrows // 2
    far = nz // 2
    r = lax.axis_index("rows")
    w = lax.axis_index("width")
    z, c = r // 2, lax.rem(r, 2)
    bounds = bounds_of(rows)
    nchunk = len(bounds)
    early_rows = bounds[0][1]
    is_root = r == ROOT

    def row_peer(i):
        return {"rows": lax.rem(r + i, nrows)}

    def width_peer(i):
        return {"width": lax.rem(w + i, nwidth)}

    ahead = (row_peer(2), row_peer(nrows - 2))
    partner = {"rows": r + 1 - 2 * c}

    barrier = pltpu.get_barrier_semaphore()
    for dz in (1, nz - 1):
        for core in (0, 1):
            pl.semaphore_signal(
                barrier, inc=1, device_id={"rows": lax.rem(z + dz, nz) * 2 + core}, device_id_type=MESH)
    pl.semaphore_signal(barrier, inc=1, device_id=partner, device_id_type=MESH)

    @pl.when(is_root)
    def _():
        for i in range(1, nwidth):
            pl.semaphore_signal(barrier, inc=1, device_id=width_peer(i), device_id_type=MESH)

    leads = [
        pltpu.make_async_copy(src, dst, lead_sem.at[i])
        for i, (src, dst) in enumerate(((mix_hbm, mix), (norm_t_hbm, norm_t), (norm_s_hbm, norm_s)))
    ]
    for copy in leads:
        copy.start()
    parts = (
        (one_q, a_buf, 0, qd), (other_q, b_buf, 0, qd),
        (one_k, a_buf, qd, kd), (other_k, b_buf, qd, kd),
        (one_v, a_buf, qd + kd, kd), (other_v, b_buf, qd + kd, kd),
    )

    def loads(step):
        span = pl.ds(step * LOAD, LOAD)
        return [
            pltpu.make_async_copy(src.at[span, :], dst.at[span, pl.ds(at, n)], in_sem.at[step, i])
            for i, (src, dst, at, n) in enumerate(parts)
        ]

    for step in range(rows // LOAD):
        for copy in loads(step):
            copy.start()
    for copy in leads:
        copy.wait()

    for at in range(0, rows, LANES):
        n = min(LANES, rows - at)
        line = mix[:, at:at + n]
        if n < LANES:
            line = jnp.concatenate([line, jnp.zeros((1, LANES - n), jnp.float32)], axis=1)
        square = jnp.transpose(jnp.broadcast_to(line, (LANES, LANES)))
        mixb[at:at + n, :] = square[:n, :]

    def early_copy(direction, piece):
        span = pl.ds(piece * LOAD, LOAD)
        return pltpu.make_async_remote_copy(
            src_ref=a_buf.at[span, :], dst_ref=early.at[direction, span, :], send_sem=early_send.at[direction, piece],
            recv_sem=early_recv.at[direction, piece], device_id=ahead[direction], device_id_type=MESH)

    acc[...] = jnp.zeros((8, cols), jnp.float32)
    for step in range(rows // LOAD):
        for copy in loads(step):
            copy.wait()
        span = slice(step * LOAD, (step + 1) * LOAD)
        m = mixb[span, :]
        rest = 1.0 - m
        for at in range(0, cols, LANES):
            lanes = slice(at, at + LANES)
            whole = m * a_buf[span, lanes] + rest * b_buf[span, lanes]
            a_buf[span, lanes] = whole
            top = jnp.max(jnp.abs(whole).reshape(LOAD // 8, 8, LANES), axis=0)
            acc[:, lanes] = jnp.maximum(acc[:, lanes], top)
        if step == 0:
            pl.semaphore_wait(barrier, 5 + jnp.where(is_root, nwidth - 1, 0))
            for direction in (0, 1):
                pl.semaphore_signal(tokens.at[direction, 2], inc=1, device_id=ahead[direction], device_id_type=MESH)
        if (step + 1) * LOAD <= early_rows:
            for direction in (0, 1):
                early_copy(direction, step).start()
    maxima[r] = jnp.max(acc[...], axis=0, keepdims=True)

    for hop in range(2, far + 1):
        for direction in (0, 1):
            pl.semaphore_wait(tokens.at[direction, hop], 1)
            if hop < far:
                pl.semaphore_signal(
                    tokens.at[direction, hop + 1], inc=1, device_id=ahead[direction], device_id_type=MESH)

    order = sorted(range(1, nrows), key=lambda i: -min(i, nrows - i))

    def max_copy(i):
        return pltpu.make_async_remote_copy(
            src_ref=maxima.at[r], dst_ref=maxima.at[r], send_sem=max_send.at[i], recv_sem=max_recv.at[i],
            device_id=row_peer(i), device_id_type=MESH)

    for i in order:
        max_copy(i).start()

    small = norm_t.shape[1]
    pos = lax.rem(r, 2) * nwidth + w
    first, lane0 = (pos * small) // LANES, lax.rem(pos * small, LANES)
    seg[...] = jnp.zeros((8, LANES), jnp.float32)
    seg[0:1, 0:small] = norm_t[...] + norm_s[...]
    turned = pltpu.roll(seg[...], lane0, 1)[0:1, :]
    lane = lax.broadcasted_iota(jnp.int32, (8, LANES), 1)
    line = lax.broadcasted_iota(jnp.int32, (8, LANES), 0)
    here = ((line == first) & (lane >= lane0)) | ((line == first + 1) & (lane < lane0))
    tiles[r] = jnp.where(here, jnp.broadcast_to(turned, (8, LANES)), 0.0)

    def tile_copy(source):
        return pltpu.make_async_remote_copy(
            src_ref=tiles.at[source], dst_ref=tiles.at[source], send_sem=tile_send, recv_sem=tile_recv.at[source],
            device_id={"rows": ROOT}, device_id_type=MESH)

    def gain_copy(i):
        return pltpu.make_async_remote_copy(
            src_ref=gains.at[w], dst_ref=gains.at[w], send_sem=gain_send.at[i], recv_sem=gain_recv.at[i],
            device_id=width_peer(i), device_id_type=MESH)

    def norm_copy(i):
        return pltpu.make_async_remote_copy(
            src_ref=norm_out, dst_ref=norm_out, send_sem=norm_send.at[i], recv_sem=norm_recv,
            device_id=row_peer(i), device_id_type=MESH)

    @pl.when(jnp.logical_not(is_root))
    def _():
        tile_copy(r).start()

    for i in order:
        max_copy(i).wait_recv()
    scale = maxima[0]
    for i in range(1, nrows):
        scale = jnp.maximum(scale, maxima[i])

    def place(direction, hop, core, chunk):
        lo, hi = bounds[chunk]
        owner = lax.rem(z - hop + nz, nz) if direction == 0 else lax.rem(z + hop, nz)
        return pl.ds(pl.multiple_of((owner * 2 + core) * rows + lo, 16), hi - lo)

    def ring(direction, hop, chunk):
        ref = out.at[place(direction, hop, c, chunk), :]
        return pltpu.make_async_remote_copy(
            src_ref=ref, dst_ref=ref, send_sem=ring_send.at[direction, hop, chunk],
            recv_sem=ring_recv.at[direction, hop, chunk], device_id=ahead[direction], device_id_type=MESH)

    def arrived(direction, hop, chunk):
        ref = out.at[place(direction, hop, c, chunk), :]
        return pltpu.make_async_remote_copy(
            src_ref=ref, dst_ref=ref, send_sem=ring_send.at[direction, hop - 1, chunk],
            recv_sem=ring_recv.at[direction, hop - 1, chunk], device_id=ahead[direction], device_id_type=MESH)

    def share(direction, hop, chunk, core):
        ref = out.at[place(direction, hop, core, chunk), :]
        return pltpu.make_async_remote_copy(
            src_ref=ref, dst_ref=ref, send_sem=share_send.at[direction, hop, chunk],
            recv_sem=share_recv.at[direction, hop, chunk], device_id=partner, device_id_type=MESH)

    def chunks(direction, hop):
        if hop < far:
            return list(range(nchunk))
        return list(range(nchunk // 2)) if direction == 0 else list(range(nchunk // 2, nchunk))

    def rounded(source, direction, hop, chunk):
        at_rows = place(direction, hop, c, chunk)
        for at in range(0, cols, LANES):
            lanes = slice(at, at + LANES)
            out[at_rows, lanes] = (source[:, lanes] / scale[:, lanes]).astype(out.dtype)

    for chunk in (*range(1, nchunk), 0):
        lo, hi = bounds[chunk]
        rounded(a_buf.at[lo:hi, :], 0, 0, chunk)
        if chunk:
            ring(0, 0, chunk).start()
            ring(1, 0, chunk).start()
        share(0, 0, chunk, c).start()
    for line in range(qd // LANES):
        scale_q[line:line + 1, :] = scale[:, line * LANES:(line + 1) * LANES]
    scale_k[...] = scale[:, qd:qd + kd]
    scale_v[...] = scale[:, qd + kd:]

    for hop in range(1, far + 1):
        for pair in zip(*(chunks(d, hop) for d in (0, 1))):
            for direction, chunk in enumerate(pair):
                if hop == 1 and chunk == 0:
                    for piece in range(early_rows // LOAD):
                        early_copy(direction, piece).wait_recv()
                    rounded(early.at[direction], direction, hop, chunk)
                else:
                    arrived(direction, hop, chunk).wait_recv()
                if hop + 1 <= far and chunk in chunks(direction, hop + 1):
                    ring(direction, hop, chunk).start()
                share(direction, hop, chunk, c).start()

        if hop == 1:
            @pl.when(is_root)
            def _():
                for i in range(nrows):
                    if i != ROOT:
                        tile_copy(i).wait_recv()
                for g in range(nrows // 2):
                    gains[w, 8 * g:8 * g + 8, :] = tiles[2 * g] + tiles[2 * g + 1]
                for i in range(1, nwidth):
                    gain_copy(i).start()
        if hop == 2:
            @pl.when(is_root)
            def _():
                for i in range(1, nwidth):
                    gain_copy(i).wait_recv()
                per = 2 * nwidth * small // LANES
                for g in range(nrows // 2):
                    full = gains[0, 8 * g:8 * g + 8, :]
                    for i in range(1, nwidth):
                        full = full + gains[i, 8 * g:8 * g + 8, :]
                    joined[g * per:(g + 1) * per, :] = full[:per, :]
                norm_out[...] = joined[...].astype(norm_out.dtype)
                for i in range(1, nrows):
                    norm_copy(i).start()

    for hop in range(far + 1):
        for direction in (0, 1) if hop else (0,):
            for chunk in chunks(direction, hop):
                share(direction, hop, chunk, 1 - c).wait_recv()
                share(direction, hop, chunk, c).wait_send()
    for hop in range(far):
        for direction in (0, 1):
            for chunk in chunks(direction, hop + 1):
                if hop or chunk:
                    ring(direction, hop, chunk).wait_send()
    for direction in (0, 1):
        for piece in range(early_rows // LOAD):
            early_copy(direction, piece).wait_send()
    for i in range(1, nrows):
        max_copy(i).wait_send()

    @pl.when(is_root)
    def _():
        for i in range(1, nwidth):
            gain_copy(i).wait_send()
        for i in range(1, nrows):
            norm_copy(i).wait_send()

    @pl.when(jnp.logical_not(is_root))
    def _():
        tile_copy(r).wait_send()
        norm_copy(1).wait_recv()


def write_kernel(dims, full, *refs):
    qd, kd = dims
    q, k, v = refs[4:7]
    sems = refs[-1]
    rows = full.shape[0]
    pieces = 8
    step = rows // pieces
    copies = []
    for i in range(pieces):
        span = pl.ds(i * step, step)
        copies.append((full.at[span, pl.ds(0, qd)], q.at[span, :]))
        copies.append((full.at[span, pl.ds(qd, kd)], k.at[span, :]))
        copies.append((full.at[span, pl.ds(qd + kd, kd)], v.at[span, :]))
    copies.extend(zip(refs[:4], refs[7:11]))
    started = [pltpu.make_async_copy(src, dst, sems.at[i]) for i, (src, dst) in enumerate(copies)]
    for copy in started:
        copy.start()
    for copy in started:
        copy.wait()


def shards(nrows, nwidth, one_q, other_q, one_k, other_k, one_v, other_v, mix, norm_t, norm_s):
    rows, qd = one_q.shape
    kd = one_k.shape[1]
    cols = qd + 2 * kd
    small = norm_t.shape[0]
    total = rows * nrows
    lines = small * nrows * nwidth // LANES
    far, nchunk = nrows // 4, len(bounds_of(rows))
    early_rows = bounds_of(rows)[0][1]
    dma = pltpu.SemaphoreType.DMA
    hbm = pl.BlockSpec(memory_space=pltpu.HBM)
    vmem = pl.BlockSpec(memory_space=pltpu.VMEM)
    full, scale_q, scale_k, scale_v, norm = pl.pallas_call(
        functools.partial(gather_kernel, nrows, nwidth, (rows, qd, kd)),
        out_shape=(
            pltpu.VMEM((total, cols), jnp.bfloat16),
            pltpu.VMEM((qd // LANES, LANES), jnp.float32),
            pltpu.VMEM((1, kd), jnp.float32),
            pltpu.VMEM((1, kd), jnp.float32),
            pltpu.VMEM((lines, LANES), jnp.bfloat16),
        ),
        in_specs=[hbm] * 9,
        out_specs=(vmem,) * 5,
        scratch_shapes=[
            pltpu.VMEM((1, rows), jnp.float32),
            pltpu.VMEM((1, small), jnp.float32),
            pltpu.VMEM((1, small), jnp.float32),
            pltpu.VMEM((rows, cols), jnp.float32),
            pltpu.VMEM((rows, cols), jnp.float32),
            pltpu.VMEM((2, early_rows, cols), jnp.float32),
            pltpu.VMEM((rows, LANES), jnp.float32),
            pltpu.VMEM((8, cols), jnp.float32),
            pltpu.VMEM((nrows, 1, cols), jnp.float32),
            pltpu.VMEM((8, LANES), jnp.float32),
            pltpu.VMEM((nrows, 8, LANES), jnp.float32),
            pltpu.VMEM((nwidth, 4 * nrows, LANES), jnp.float32),
            pltpu.VMEM((lines, LANES), jnp.float32),
            pltpu.SemaphoreType.REGULAR((2, far + 1)),
            dma((3,)),
            dma((rows // LOAD, 6)),
            dma((nrows,)),
            dma((nrows,)),
            dma(()),
            dma((nrows,)),
            dma((nwidth,)),
            dma((nwidth,)),
            dma((nrows,)),
            dma(()),
            dma((2, early_rows // LOAD)),
            dma((2, early_rows // LOAD)),
            dma((2, far, nchunk)),
            dma((2, far, nchunk)),
            dma((2, far + 1, nchunk)),
            dma((2, far + 1, nchunk)),
        ],
        compiler_params=pltpu.CompilerParams(
            collective_id=0, has_side_effects=True, vmem_limit_bytes=24 * 1024 * 1024),
        name="gather",
    )(*(pltpu.with_memory_space_constraint(x, pltpu.HBM) for x in (
        one_q, other_q, one_k, other_k, one_v, other_v,
        mix.reshape(1, -1), norm_t.reshape(1, -1), norm_s.reshape(1, -1))))
    q, k, v, scale_q, scale_k, scale_v, norm_o = pl.pallas_call(
        functools.partial(write_kernel, (qd, kd)),
        out_shape=(
            jax.ShapeDtypeStruct((total, qd), jnp.bfloat16),
            jax.ShapeDtypeStruct((total, kd), jnp.bfloat16),
            jax.ShapeDtypeStruct((total, kd), jnp.bfloat16),
            jax.ShapeDtypeStruct((qd // LANES, LANES), jnp.float32),
            jax.ShapeDtypeStruct((1, kd), jnp.float32),
            jax.ShapeDtypeStruct((1, kd), jnp.float32),
            jax.ShapeDtypeStruct((lines, LANES), jnp.bfloat16),
        ),
        in_specs=[vmem] * 5,
        out_specs=(hbm,) * 7,
        scratch_shapes=[pltpu.SemaphoreType.DMA((28,))],
        compiler_params=pltpu.CompilerParams(vmem_limit_bytes=1024 * 1024),
        name="write",
    )(full, scale_q, scale_k, scale_v, norm)
    return (q, k, v, scale_q.reshape(-1), scale_k.reshape(-1), scale_v.reshape(-1),
            norm_o.reshape(-1))


def solution(mesh):
    rows = ("site", "rows")
    return jax.shard_map(
        functools.partial(shards, mesh.shape["rows"], mesh.shape["width"]),
        mesh=mesh,
        in_specs=(P(rows, "width"),) * 6 + (P(rows), P(("site", "rows", "width")), P(("site", "rows", "width"))),
        out_specs=(P("site", "width"),) * 3 + (P(("site", "width")),) * 3 + (P("site"),),
        check_vma=False,
    )
```

```python
import functools

import jax
import jax.numpy as jnp
from jax import lax
from jax.experimental import pallas as pl
from jax.experimental.pallas import tpu as pltpu
from jax.sharding import PartitionSpec as P

MESH = pl.DeviceIdType.MESH
LANES = 128
LOAD = 112
ROOT = 1
EARLY = 1
CUT = 48


def bounds_of(rows):
    half = rows // 2
    cuts = [0, CUT, half]
    cuts += [half + at for at in cuts[1:]]
    return list(zip(cuts, cuts[1:]))


def gather_kernel(nrows, nwidth, dims, *refs):
    (one_q, other_q, one_k, other_k, one_v, other_v, mix_hbm, norm_t_hbm, norm_s_hbm,
     out, scale_q, scale_k, scale_v, norm_out,
     mix, norm_t, norm_s, a_buf, b_buf, early, mixb, acc, maxima, seg, tiles, gains, joined,
     lead_sem, in_sem, max_send, max_recv, tile_send, tile_recv, gain_send, gain_recv, norm_send, norm_recv,
     early_send, early_recv, ring_send, ring_recv, share_send, share_recv) = refs
    rows, qd, kd = dims
    cols = qd + 2 * kd
    nz = nrows // 2
    far = nz // 2
    r = lax.axis_index("rows")
    w = lax.axis_index("width")
    z, c = r // 2, lax.rem(r, 2)
    bounds = bounds_of(rows)
    nchunk = len(bounds)
    is_root = r == ROOT

    def row_peer(i):
        return {"rows": lax.rem(r + i, nrows)}

    def width_peer(i):
        return {"width": lax.rem(w + i, nwidth)}

    ahead = (row_peer(2), row_peer(nrows - 2))
    partner = {"rows": r + 1 - 2 * c}
    farthest_first = sorted(range(1, nrows), key=lambda i: -min(i, nrows - i))

    barrier = pltpu.get_barrier_semaphore()
    for i in farthest_first:
        pl.semaphore_signal(barrier, inc=1, device_id=row_peer(i), device_id_type=MESH)

    @pl.when(is_root)
    def _():
        for i in range(1, nwidth):
            pl.semaphore_signal(barrier, inc=1, device_id=width_peer(i), device_id_type=MESH)

    leads = [
        pltpu.make_async_copy(src, dst, lead_sem.at[i])
        for i, (src, dst) in enumerate(((mix_hbm, mix), (norm_t_hbm, norm_t), (norm_s_hbm, norm_s)))
    ]
    for copy in leads:
        copy.start(priority=1)
    parts = (
        (one_q, a_buf, 0, qd), (other_q, b_buf, 0, qd),
        (one_k, a_buf, qd, kd), (other_k, b_buf, qd, kd),
        (one_v, a_buf, qd + kd, kd), (other_v, b_buf, qd + kd, kd),
    )

    def loads(step):
        span = pl.ds(step * LOAD, LOAD)
        return [
            pltpu.make_async_copy(src.at[span, :], dst.at[span, pl.ds(at, n)], in_sem.at[step])
            for src, dst, at, n in parts
        ]

    for step in range(rows // LOAD):
        for copy in loads(step):
            copy.start()
    for copy in leads:
        copy.wait()

    for at in range(0, rows, LANES):
        n = min(LANES, rows - at)
        line = mix[:, at:at + n]
        if n < LANES:
            line = jnp.concatenate([line, jnp.zeros((1, LANES - n), jnp.float32)], axis=1)
        square = jnp.transpose(jnp.broadcast_to(line, (LANES, LANES)))
        mixb[at:at + n, :] = square[:n, :]

    acc[...] = jnp.zeros((8, cols), jnp.float32)
    for step in range(rows // LOAD):
        both = a_buf.at[pl.ds(0, 2 * LOAD), :]
        pltpu.make_async_copy(both, both, in_sem.at[step]).wait()
        span = slice(step * LOAD, (step + 1) * LOAD)
        m = mixb[span, :]
        rest = 1.0 - m
        for at in range(0, cols, LANES):
            lanes = slice(at, at + LANES)
            whole = m * a_buf[span, lanes] + rest * b_buf[span, lanes]
            a_buf[span, lanes] = whole
            top = jnp.max(jnp.abs(whole).reshape(LOAD // 8, 8, LANES), axis=0)
            acc[:, lanes] = jnp.maximum(acc[:, lanes], top)
    maxima[r] = jnp.max(acc[...], axis=0, keepdims=True)

    pl.semaphore_wait(barrier, nrows - 1 + jnp.where(is_root, nwidth - 1, 0))

    def max_copy(i):
        return pltpu.make_async_remote_copy(
            src_ref=maxima.at[r], dst_ref=maxima.at[r], send_sem=max_send, recv_sem=max_recv,
            device_id=row_peer(i), device_id_type=MESH)

    def all_of(ref, count, send_sem, recv_sem):
        part = ref.at[pl.ds(0, count)]
        return pltpu.make_async_remote_copy(
            src_ref=part, dst_ref=part, send_sem=send_sem, recv_sem=recv_sem, device_id=partner, device_id_type=MESH)

    for i in farthest_first:
        max_copy(i).start()

    def early_copy(direction, chunk):
        span = pl.ds(bounds[chunk][0], bounds[chunk][1] - bounds[chunk][0])
        return pltpu.make_async_remote_copy(
            src_ref=a_buf.at[span, :], dst_ref=early.at[direction, span, :], send_sem=early_send,
            recv_sem=early_recv.at[direction, chunk], device_id=ahead[direction], device_id_type=MESH)

    for chunk in range(EARLY):
        for direction in (0, 1):
            early_copy(direction, chunk).start()

    small = norm_t.shape[1]
    pos = lax.rem(r, 2) * nwidth + w
    first, lane0 = (pos * small) // LANES, lax.rem(pos * small, LANES)
    seg[...] = jnp.zeros((8, LANES), jnp.float32)
    seg[0:1, 0:small] = norm_t[...] + norm_s[...]
    turned = pltpu.roll(seg[...], lane0, 1)[0:1, :]
    lane = lax.broadcasted_iota(jnp.int32, (8, LANES), 1)
    line = lax.broadcasted_iota(jnp.int32, (8, LANES), 0)
    here = ((line == first) & (lane >= lane0)) | ((line == first + 1) & (lane < lane0))
    tiles[r] = jnp.where(here, jnp.broadcast_to(turned, (8, LANES)), 0.0)

    def tile_copy(source):
        return pltpu.make_async_remote_copy(
            src_ref=tiles.at[source], dst_ref=tiles.at[source], send_sem=tile_send, recv_sem=tile_recv,
            device_id={"rows": ROOT}, device_id_type=MESH)

    def gain_copy(i):
        return pltpu.make_async_remote_copy(
            src_ref=gains.at[w], dst_ref=gains.at[w], send_sem=gain_send, recv_sem=gain_recv,
            device_id=width_peer(i), device_id_type=MESH)

    def norm_copy(i):
        return pltpu.make_async_remote_copy(
            src_ref=norm_out, dst_ref=norm_out, send_sem=norm_send, recv_sem=norm_recv,
            device_id=row_peer(i), device_id_type=MESH)

    @pl.when(jnp.logical_not(is_root))
    def _():
        tile_copy(r).start()

    all_of(maxima, nrows - 1, max_send, max_recv).wait_recv()
    scale = maxima[0]
    for i in range(1, nrows):
        scale = jnp.maximum(scale, maxima[i])

    def place(direction, hop, chunk):
        lo, hi = bounds[chunk]
        owner = lax.rem(z - hop + nz, nz) if direction == 0 else lax.rem(z + hop, nz)
        return pl.ds(pl.multiple_of((owner * 2 + c) * rows + lo, 16), hi - lo)

    def landing(direction, hop, chunk):
        return (2 * hop + direction) * nchunk + chunk if hop + 1 < far else 2 * hop * nchunk + chunk

    def ring(direction, hop, chunk):
        ref = out.at[place(direction, hop, chunk), :]
        return pltpu.make_async_remote_copy(
            src_ref=ref, dst_ref=ref, send_sem=ring_send, recv_sem=ring_recv.at[landing(direction, hop, chunk)],
            device_id=ahead[direction], device_id_type=MESH)

    def arrived(direction, hop, chunk):
        ref = out.at[place(direction, hop, chunk), :]
        return pltpu.make_async_remote_copy(
            src_ref=ref, dst_ref=ref, send_sem=ring_send, recv_sem=ring_recv.at[landing(direction, hop - 1, chunk)],
            device_id=ahead[direction], device_id_type=MESH)

    def share(direction, hop, chunk):
        ref = out.at[place(direction, hop, chunk), :]
        return pltpu.make_async_remote_copy(
            src_ref=ref, dst_ref=ref, send_sem=share_send, recv_sem=share_recv,
            device_id=partner, device_id_type=MESH)

    def chunks(direction, hop):
        if hop < far:
            return [0, 1, 3, 2] if hop == 1 else [1, 0, 3, 2]
        return [1, 0] if direction == 0 else [3, 2]

    def rounded(source, direction, hop, chunk):
        at_rows = place(direction, hop, chunk)
        for at in range(0, cols, LANES):
            lanes = slice(at, at + LANES)
            out[at_rows, lanes] = (source[:, lanes] / scale[:, lanes]).astype(out.dtype)

    for chunk in (1, 3, 2, 0):
        lo, hi = bounds[chunk]
        rounded(a_buf.at[lo:hi, :], 0, 0, chunk)
        if chunk >= EARLY:
            for direction in (0, 1):
                ring(direction, 0, chunk).start()
        share(0, 0, chunk).start()
    for line in range(qd // LANES):
        scale_q[line:line + 1, :] = scale[:, line * LANES:(line + 1) * LANES]
    scale_k[...] = scale[:, qd:qd + kd]
    scale_v[...] = scale[:, qd + kd:]

    for hop in range(1, far + 1):
        for step in zip(*(chunks(d, hop) for d in (0, 1))):
            for direction, chunk in enumerate(step):
                if hop == 1 and chunk < EARLY:
                    early_copy(direction, chunk).wait_recv()
                    rounded(early.at[direction, bounds[chunk][0]:bounds[chunk][1], :], direction, hop, chunk)
                else:
                    arrived(direction, hop, chunk).wait_recv()
                if hop + 1 <= far and chunk in chunks(direction, hop + 1):
                    ring(direction, hop, chunk).start()
                share(direction, hop, chunk).start()

        if hop == 1:
            @pl.when(is_root)
            def _():
                all_of(tiles, nrows - 1, tile_send, tile_recv).wait_recv()
                for g in range(nrows // 2):
                    gains[w, 8 * g:8 * g + 8, :] = tiles[2 * g] + tiles[2 * g + 1]
                for i in range(1, nwidth):
                    gain_copy(i).start()
        if hop == 2:
            @pl.when(is_root)
            def _():
                all_of(gains, nwidth - 1, gain_send, gain_recv).wait_recv()
                per = 2 * nwidth * small // LANES
                for g in range(nrows // 2):
                    full = gains[0, 8 * g:8 * g + 8, :]
                    for i in range(1, nwidth):
                        full = full + gains[i, 8 * g:8 * g + 8, :]
                    joined[g * per:(g + 1) * per, :] = full[:per, :]
                norm_out[...] = joined[...].astype(norm_out.dtype)
                for i in range(1, nrows):
                    norm_copy(i).start()

    all_of(out, nz * rows, share_send, share_recv).wait_recv()
    all_of(out, nz * rows, share_send, share_recv).wait_send()
    all_of(out, (nz - 1) * rows - 2 * bounds[EARLY - 1][1], ring_send, ring_recv.at[0]).wait_send()
    for chunk in range(EARLY):
        for direction in (0, 1):
            early_copy(direction, chunk).wait_send()
    all_of(maxima, nrows - 1, max_send, max_recv).wait_send()

    @pl.when(is_root)
    def _():
        all_of(gains, nwidth - 1, gain_send, gain_recv).wait_send()
        for i in range(1, nrows):
            norm_copy(i).wait_send()

    @pl.when(jnp.logical_not(is_root))
    def _():
        tile_copy(r).wait_send()
        norm_copy(1).wait_recv()


def write_kernel(dims, full, *refs):
    qd, kd = dims
    q, k, v = refs[4:7]
    sems = refs[-1]
    half = full.shape[0] // 2
    started = []
    for i in range(2):
        span = pl.ds(i * half, half)
        for j, (o, at, n) in enumerate(((q, 0, qd), (k, qd, kd), (v, qd + kd, kd))):
            started.append((i, pltpu.make_async_copy(full.at[span, pl.ds(at, n)], o.at[span, :], sems.at[4 + 3 * i + j])))
    started += [(1, pltpu.make_async_copy(src, dst, sems.at[i])) for i, (src, dst) in enumerate(zip(refs[:4], refs[7:11]))]
    for i, copy in started:
        copy.start(priority=i)
    for i, copy in started:
        copy.wait()


def shards(nrows, nwidth, one_q, other_q, one_k, other_k, one_v, other_v, mix, norm_t, norm_s):
    rows, qd = one_q.shape
    kd = one_k.shape[1]
    cols = qd + 2 * kd
    small = norm_t.shape[0]
    total = rows * nrows
    lines = small * nrows * nwidth // LANES
    far, nchunk = nrows // 4, len(bounds_of(rows))
    early_rows = bounds_of(rows)[EARLY - 1][1]
    dma = pltpu.SemaphoreType.DMA
    hbm = pl.BlockSpec(memory_space=pltpu.HBM)
    vmem = pl.BlockSpec(memory_space=pltpu.VMEM)
    full, scale_q, scale_k, scale_v, norm = pl.pallas_call(
        functools.partial(gather_kernel, nrows, nwidth, (rows, qd, kd)),
        out_shape=(
            pltpu.VMEM((total, cols), jnp.bfloat16),
            pltpu.VMEM((qd // LANES, LANES), jnp.float32),
            pltpu.VMEM((1, kd), jnp.float32),
            pltpu.VMEM((1, kd), jnp.float32),
            pltpu.VMEM((lines, LANES), jnp.bfloat16),
        ),
        in_specs=[hbm] * 9,
        out_specs=(vmem,) * 5,
        scratch_shapes=[
            pltpu.VMEM((1, rows), jnp.float32),
            pltpu.VMEM((1, small), jnp.float32),
            pltpu.VMEM((1, small), jnp.float32),
            pltpu.VMEM((rows, cols), jnp.float32),
            pltpu.VMEM((rows, cols), jnp.float32),
            pltpu.VMEM((2, early_rows, cols), jnp.float32),
            pltpu.VMEM((rows, LANES), jnp.float32),
            pltpu.VMEM((8, cols), jnp.float32),
            pltpu.VMEM((nrows, 1, cols), jnp.float32),
            pltpu.VMEM((8, LANES), jnp.float32),
            pltpu.VMEM((nrows, 8, LANES), jnp.float32),
            pltpu.VMEM((nwidth, 4 * nrows, LANES), jnp.float32),
            pltpu.VMEM((lines, LANES), jnp.float32),
            dma((3,)),
            dma((rows // LOAD,)),
            dma(()),
            dma(()),
            dma(()),
            dma(()),
            dma(()),
            dma(()),
            dma(()),
            dma(()),
            dma(()),
            dma((2, EARLY)),
            dma(()),
            dma((2 * (far - 1) * nchunk + nchunk,)),
            dma(()),
            dma(()),
        ],
        compiler_params=pltpu.CompilerParams(
            collective_id=0, has_side_effects=True, vmem_limit_bytes=24 * 1024 * 1024),
        name="gather",
    )(*(pltpu.with_memory_space_constraint(x, pltpu.HBM) for x in (
        one_q, other_q, one_k, other_k, one_v, other_v,
        mix.reshape(1, -1), norm_t.reshape(1, -1), norm_s.reshape(1, -1))))
    q, k, v, scale_q, scale_k, scale_v, norm_o = pl.pallas_call(
        functools.partial(write_kernel, (qd, kd)),
        out_shape=(
            jax.ShapeDtypeStruct((total, qd), jnp.bfloat16),
            jax.ShapeDtypeStruct((total, kd), jnp.bfloat16),
            jax.ShapeDtypeStruct((total, kd), jnp.bfloat16),
            jax.ShapeDtypeStruct((qd // LANES, LANES), jnp.float32),
            jax.ShapeDtypeStruct((1, kd), jnp.float32),
            jax.ShapeDtypeStruct((1, kd), jnp.float32),
            jax.ShapeDtypeStruct((lines, LANES), jnp.bfloat16),
        ),
        in_specs=[vmem] * 5,
        out_specs=(hbm,) * 7,
        scratch_shapes=[dma((10,))],
        compiler_params=pltpu.CompilerParams(vmem_limit_bytes=1024 * 1024),
        name="write",
    )(full, scale_q, scale_k, scale_v, norm)
    return (q, k, v, scale_q.reshape(-1), scale_k.reshape(-1), scale_v.reshape(-1),
            norm_o.reshape(-1))


def solution(mesh):
    rows = ("site", "rows")
    return jax.shard_map(
        functools.partial(shards, mesh.shape["rows"], mesh.shape["width"]),
        mesh=mesh,
        in_specs=(P(rows, "width"),) * 6 + (P(rows), P(("site", "rows", "width")), P(("site", "rows", "width"))),
        out_specs=(P("site", "width"),) * 3 + (P(("site", "width")),) * 3 + (P("site"),),
        check_vma=False,
    )
```

```python
import functools

import jax
import jax.numpy as jnp
from jax import lax
from jax.experimental import pallas as pl
from jax.experimental.pallas import tpu as pltpu
from jax.sharding import PartitionSpec as P

MESH = pl.DeviceIdType.MESH
LANES = 128
LOAD = 64
EARLY = 4
CUTS = (64, 112, 192)
TINY = 1e-30


def bounds_of(rows):
    half = rows // 2
    cuts = [0, *CUTS, half]
    cuts += [half + at for at in cuts[1:]]
    return list(zip(cuts, cuts[1:]))


def gather_kernel(nrows, nwidth, dims, *refs):
    (one_q, other_q, one_k, other_k, one_v, other_v, mix_hbm, norm_t_hbm, norm_s_hbm,
     out, scale_q, scale_k, scale_v, norm_out,
     mix, norm_t, norm_s, a_buf, b_buf, early, mixb, acc, firsts, pair, maxima, seg, tiles, gains, joined,
     tokens, lead_sem, in_sem, first_send, first_recv, pair_send, pair_recv, max_send, max_recv, tile_send, tile_recv, gain_send, gain_recv, norm_send, norm_recv,
     early_send, early_recv, ring_send, ring_recv, share_send, share_recv) = refs
    rows, qd, kd = dims
    cols = qd + 2 * kd
    nz = nrows // 2
    far = nz // 2
    r = lax.axis_index("rows")
    w = lax.axis_index("width")
    z, c = r // 2, lax.rem(r, 2)
    bounds = bounds_of(rows)
    nchunk = len(bounds)
    root = nrows // 2 + 1
    is_root = r == root

    def row_peer(i):
        return {"rows": lax.rem(r + i, nrows)}

    def width_peer(i):
        return {"width": lax.rem(w + i, nwidth)}

    ahead = (row_peer(2), row_peer(nrows - 2))
    partner = {"rows": r + 1 - 2 * c}
    farthest_first = sorted(range(1, nz), key=lambda i: -min(i, nz - i))

    barrier = pltpu.get_barrier_semaphore()
    for dz in (1, nz - 1):
        for core in (0, 1):
            pl.semaphore_signal(
                barrier, inc=1, device_id={"rows": lax.rem(z + dz, nz) * 2 + core}, device_id_type=MESH)
    pl.semaphore_signal(barrier, inc=1, device_id=partner, device_id_type=MESH)

    @pl.when(is_root)
    def _():
        for i in range(1, nwidth):
            pl.semaphore_signal(barrier, inc=1, device_id=width_peer(i), device_id_type=MESH)

    leads = [
        pltpu.make_async_copy(src, dst, lead_sem.at[i])
        for i, (src, dst) in enumerate(((mix_hbm, mix), (norm_t_hbm, norm_t), (norm_s_hbm, norm_s)))
    ]
    for copy in leads:
        copy.start(priority=1)
    parts = (
        (one_q, a_buf, 0, qd), (other_q, b_buf, 0, qd),
        (one_k, a_buf, qd, kd), (other_k, b_buf, qd, kd),
        (one_v, a_buf, qd + kd, kd), (other_v, b_buf, qd + kd, kd),
    )

    def loads(step):
        span = pl.ds(step * LOAD, LOAD)
        return [
            pltpu.make_async_copy(src.at[span, :], dst.at[span, pl.ds(at, n)], in_sem.at[step])
            for src, dst, at, n in parts
        ]

    def wait_load(step):
        both = a_buf.at[pl.ds(0, 2 * LOAD), :]
        pltpu.make_async_copy(both, both, in_sem.at[step]).wait()

    def spread(at):
        n = min(LANES, rows - at)
        line = mix[:, at:at + n]
        if n < LANES:
            line = jnp.concatenate([line, jnp.zeros((1, LANES - n), jnp.float32)], axis=1)
        square = jnp.transpose(jnp.broadcast_to(line, (LANES, LANES)))
        mixb[at:at + n, :] = square[:n, :]

    def mixed(step):
        span = slice(step * LOAD, (step + 1) * LOAD)
        m = mixb[span, :]
        rest = 1.0 - m
        for at in range(0, cols, LANES):
            lanes = slice(at, at + LANES)
            whole = m * a_buf[span, lanes] + rest * b_buf[span, lanes]
            a_buf[span, lanes] = whole
            top = jnp.max(jnp.abs(whole).reshape(LOAD // 8, 8, LANES), axis=0)
            acc[:, lanes] = top if step == 0 else jnp.maximum(acc[:, lanes], top)

    def coded(chunk, own):
        inverse = 1.0 / jnp.maximum(own, TINY)
        span = slice(*bounds[chunk])
        for at in range(0, cols, LANES):
            lanes = slice(at, at + LANES)
            v = a_buf[span, lanes] * inverse[:, lanes]
            v2 = v * v
            v4 = v2 * v2
            v8 = v4 * v4 * 2.0**63
            code = v8 * v8
            early[2, span, lanes] = jnp.where(v < 0.0, -code, code).astype(early.dtype)

    def early_copy(direction, chunk):
        span = pl.ds(bounds[chunk][0], bounds[chunk][1] - bounds[chunk][0])
        return pltpu.make_async_remote_copy(
            src_ref=early.at[2, span, :], dst_ref=early.at[direction, span, :], send_sem=early_send,
            recv_sem=early_recv.at[direction, chunk], device_id=ahead[direction], device_id_type=MESH)

    def first_copy(direction, part):
        return pltpu.make_async_remote_copy(
            src_ref=firsts.at[2, part], dst_ref=firsts.at[direction, part], send_sem=first_send,
            recv_sem=first_recv.at[direction, part], device_id=ahead[direction], device_id_type=MESH)

    for copy in loads(0):
        copy.start()
    for copy in leads:
        copy.wait()
    wait_load(0)
    for step in range(1, rows // LOAD):
        for copy in loads(step):
            copy.start()
    spread(0)
    mixed(0)
    firsts[2, 0] = jnp.max(acc[...], axis=0, keepdims=True)
    coded(0, firsts[2, 0])

    pl.semaphore_wait(barrier, 5 + jnp.where(is_root, nwidth - 1, 0))
    for direction in (0, 1):
        early_copy(direction, 0).start()

    def tell(direction, hop):
        pl.semaphore_signal(tokens.at[direction, hop - 2], inc=1, device_id=ahead[direction], device_id_type=MESH)

    def heard(hop):
        for direction in (0, 1) if hop < far else (0,):
            pl.semaphore_wait(tokens.at[direction, hop - 2], 1)
            if hop + 1 < far or (hop < far and direction == 0):
                tell(direction, hop + 1)

    for direction in (0, 1) if far > 2 else (0,):
        tell(direction, 2)
    for direction in (0, 1):
        first_copy(direction, 0).start()
    heard(2)

    for at in range(LANES, rows, LANES):
        spread(at)
    for step in range(1, rows // LOAD):
        wait_load(step)
        mixed(step)

    def pair_copy(core):
        return pltpu.make_async_remote_copy(
            src_ref=pair.at[core], dst_ref=pair.at[core], send_sem=pair_send, recv_sem=pair_recv,
            device_id=partner, device_id_type=MESH)

    firsts[2, 1] = jnp.max(acc[...], axis=0, keepdims=True)
    pair[c] = firsts[2, 1]
    pair_copy(c).start()
    coded(1, firsts[2, 1])
    for direction in (0, 1):
        first_copy(direction, 1).start()
        early_copy(direction, 1).start()
    for hop in range(3, far + 1):
        heard(hop)
    pair_copy(1 - c).wait_recv()
    maxima[z] = jnp.maximum(pair[0], pair[1])

    def max_copy(i):
        return pltpu.make_async_remote_copy(
            src_ref=maxima.at[z], dst_ref=maxima.at[z], send_sem=max_send, recv_sem=max_recv,
            device_id=row_peer(2 * i), device_id_type=MESH)

    def all_of(ref, count, send_sem, recv_sem):
        part = ref.at[pl.ds(0, count)]
        return pltpu.make_async_remote_copy(
            src_ref=part, dst_ref=part, send_sem=send_sem, recv_sem=recv_sem, device_id=partner, device_id_type=MESH)

    for i in farthest_first:
        max_copy(i).start()
    for chunk in range(2, EARLY):
        coded(chunk, firsts[2, 1])
        for direction in (0, 1):
            early_copy(direction, chunk).start()

    small = norm_t.shape[1]
    pos = lax.rem(r, 2) * nwidth + w
    first, lane0 = (pos * small) // LANES, lax.rem(pos * small, LANES)
    seg[...] = jnp.zeros((8, LANES), jnp.float32)
    seg[0:1, 0:small] = norm_t[...] + norm_s[...]
    turned = pltpu.roll(seg[...], lane0, 1)[0:1, :]
    lane = lax.broadcasted_iota(jnp.int32, (8, LANES), 1)
    line = lax.broadcasted_iota(jnp.int32, (8, LANES), 0)
    here = ((line == first) & (lane >= lane0)) | ((line == first + 1) & (lane < lane0))
    tiles[r] = jnp.where(here, jnp.broadcast_to(turned, (8, LANES)), 0.0)

    def tile_copy(source):
        return pltpu.make_async_remote_copy(
            src_ref=tiles.at[source], dst_ref=tiles.at[source], send_sem=tile_send, recv_sem=tile_recv,
            device_id={"rows": root}, device_id_type=MESH)

    def gain_copy(i):
        return pltpu.make_async_remote_copy(
            src_ref=gains.at[w], dst_ref=gains.at[w], send_sem=gain_send, recv_sem=gain_recv,
            device_id=width_peer(i), device_id_type=MESH)

    def norm_copy(i):
        return pltpu.make_async_remote_copy(
            src_ref=norm_out, dst_ref=norm_out, send_sem=norm_send, recv_sem=norm_recv,
            device_id=row_peer(i), device_id_type=MESH)

    @pl.when(jnp.logical_not(is_root))
    def _():
        tile_copy(r).start()

    all_of(maxima, nz - 1, max_send, max_recv).wait_recv()
    scale = maxima[0]
    for i in range(1, nz):
        scale = jnp.maximum(scale, maxima[i])

    def place(direction, hop, chunk):
        lo, hi = bounds[chunk]
        owner = lax.rem(z - hop + nz, nz) if direction == 0 else lax.rem(z + hop, nz)
        return pl.ds(pl.multiple_of((owner * 2 + c) * rows + lo, 16), hi - lo)

    def landing(hop, chunk):
        return hop * nchunk + chunk - EARLY

    def ring(direction, hop, chunk):
        ref = out.at[place(direction, hop, chunk), :]
        return pltpu.make_async_remote_copy(
            src_ref=ref, dst_ref=ref, send_sem=ring_send, recv_sem=ring_recv.at[landing(hop, chunk)],
            device_id=ahead[direction], device_id_type=MESH)

    def arrived(hop, chunk):
        lo, hi = bounds[chunk]
        sides = 2 if hop < far else 1
        all_of(out, sides * (hi - lo), ring_send, ring_recv.at[landing(hop - 1, chunk)]).wait_recv()

    def share(direction, hop, chunk):
        ref = out.at[place(direction, hop, chunk), :]
        return pltpu.make_async_remote_copy(
            src_ref=ref, dst_ref=ref, send_sem=share_send, recv_sem=share_recv,
            device_id=partner, device_id_type=MESH)

    def chunks(direction, hop):
        if hop < far:
            return list(range(nchunk))
        return list(range(nchunk // 2)) if direction == 0 else list(range(nchunk // 2, nchunk))

    def rounded(source, direction, hop, chunk):
        at_rows = place(direction, hop, chunk)
        for at in range(0, cols, LANES):
            lanes = slice(at, at + LANES)
            out[at_rows, lanes] = (source[:, lanes] / scale[:, lanes]).astype(out.dtype)

    def decoded(direction, chunk):
        part = min(chunk, 1)
        if chunk < 2:
            first_copy(direction, part).wait_recv()
        factor = jnp.maximum(firsts[direction, part], TINY) / scale
        at_rows = place(direction, 1, chunk)
        for at in range(0, cols, LANES):
            lanes = slice(at, at + LANES)
            code = early[direction, bounds[chunk][0]:bounds[chunk][1], lanes].astype(jnp.float32)
            size = jnp.exp2(jnp.log2(jnp.abs(code)) * (1.0 / 16.0) - 126.0 / 16.0)
            out[at_rows, lanes] = (jnp.where(code < 0.0, -size, size) * factor[:, lanes]).astype(out.dtype)

    for chunk in (*range(EARLY, nchunk), *range(EARLY)):
        lo, hi = bounds[chunk]
        rounded(a_buf.at[lo:hi, :], 0, 0, chunk)
        if chunk >= EARLY:
            for direction in (0, 1):
                ring(direction, 0, chunk).start()
        share(0, 0, chunk).start()
    for line in range(qd // LANES):
        scale_q[line:line + 1, :] = scale[:, line * LANES:(line + 1) * LANES]
    scale_k[...] = scale[:, qd:qd + kd]
    scale_v[...] = scale[:, qd + kd:]

    for hop in range(1, far + 1):
        for step in zip(*(chunks(d, hop) for d in (0, 1))):
            for direction, chunk in enumerate(step):
                if hop == far or (direction == 0 and (hop > 1 or chunk >= EARLY)):
                    arrived(hop, chunk)
                if hop == 1 and chunk < EARLY:
                    early_copy(direction, chunk).wait_recv()
                    decoded(direction, chunk)
                if hop + 1 <= far and chunk in chunks(direction, hop + 1):
                    ring(direction, hop, chunk).start()
                share(direction, hop, chunk).start()

        if hop == 1:
            @pl.when(is_root)
            def _():
                all_of(tiles, nrows - 1, tile_send, tile_recv).wait_recv()
                for g in range(nrows // 2):
                    gains[w, 8 * g:8 * g + 8, :] = tiles[2 * g] + tiles[2 * g + 1]
                for i in range(1, nwidth):
                    gain_copy(i).start()
        if hop == 2:
            @pl.when(is_root)
            def _():
                all_of(gains, nwidth - 1, gain_send, gain_recv).wait_recv()
                per = 2 * nwidth * small // LANES
                for g in range(nrows // 2):
                    full = gains[0, 8 * g:8 * g + 8, :]
                    for i in range(1, nwidth):
                        full = full + gains[i, 8 * g:8 * g + 8, :]
                    joined[g * per:(g + 1) * per, :] = full[:per, :]
                norm_out[...] = joined[...].astype(norm_out.dtype)
                for i in range(1, nrows):
                    norm_copy(i).start()

    all_of(out, nz * rows, share_send, share_recv).wait_recv()
    all_of(out, nz * rows, share_send, share_recv).wait_send()
    all_of(out, (nz - 1) * rows - 2 * bounds[EARLY - 1][1], ring_send, ring_recv.at[0]).wait_send()
    for direction in (0, 1):
        for part in (0, 1):
            first_copy(direction, part).wait_send()
        for chunk in range(EARLY):
            early_copy(direction, chunk).wait_send()
    pair_copy(c).wait_send()
    all_of(maxima, nz - 1, max_send, max_recv).wait_send()

    @pl.when(is_root)
    def _():
        all_of(gains, nwidth - 1, gain_send, gain_recv).wait_send()
        for i in range(1, nrows):
            norm_copy(i).wait_send()

    @pl.when(jnp.logical_not(is_root))
    def _():
        tile_copy(r).wait_send()
        norm_copy(1).wait_recv()


def write_kernel(dims, full, *refs):
    qd, kd = dims
    q, k, v = refs[4:7]
    sems = refs[-1]
    half = full.shape[0] // 2
    started = []
    for i in range(2):
        span = pl.ds(i * half, half)
        for j, (o, at, n) in enumerate(((q, 0, qd), (k, qd, kd), (v, qd + kd, kd))):
            started.append((i, pltpu.make_async_copy(full.at[span, pl.ds(at, n)], o.at[span, :], sems.at[4 + 3 * i + j])))
    started += [(1, pltpu.make_async_copy(src, dst, sems.at[i])) for i, (src, dst) in enumerate(zip(refs[:4], refs[7:11]))]
    for i, copy in started:
        copy.start(priority=i)
    for i, copy in started:
        copy.wait()


def shards(nrows, nwidth, one_q, other_q, one_k, other_k, one_v, other_v, mix, norm_t, norm_s):
    rows, qd = one_q.shape
    kd = one_k.shape[1]
    cols = qd + 2 * kd
    small = norm_t.shape[0]
    total = rows * nrows
    lines = small * nrows * nwidth // LANES
    far, nchunk = nrows // 4, len(bounds_of(rows))
    early_rows = bounds_of(rows)[EARLY - 1][1]
    dma = pltpu.SemaphoreType.DMA
    hbm = pl.BlockSpec(memory_space=pltpu.HBM)
    vmem = pl.BlockSpec(memory_space=pltpu.VMEM)
    full, scale_q, scale_k, scale_v, norm = pl.pallas_call(
        functools.partial(gather_kernel, nrows, nwidth, (rows, qd, kd)),
        out_shape=(
            pltpu.VMEM((total, cols), jnp.bfloat16),
            pltpu.VMEM((qd // LANES, LANES), jnp.float32),
            pltpu.VMEM((1, kd), jnp.float32),
            pltpu.VMEM((1, kd), jnp.float32),
            pltpu.VMEM((lines, LANES), jnp.bfloat16),
        ),
        in_specs=[hbm] * 9,
        out_specs=(vmem,) * 5,
        scratch_shapes=[
            pltpu.VMEM((1, rows), jnp.float32),
            pltpu.VMEM((1, small), jnp.float32),
            pltpu.VMEM((1, small), jnp.float32),
            pltpu.VMEM((rows, cols), jnp.float32),
            pltpu.VMEM((rows, cols), jnp.float32),
            pltpu.VMEM((3, early_rows, cols), jnp.bfloat16),
            pltpu.VMEM((rows, LANES), jnp.float32),
            pltpu.VMEM((8, cols), jnp.float32),
            pltpu.VMEM((3, 2, 1, cols), jnp.float32),
            pltpu.VMEM((2, 1, cols), jnp.float32),
            pltpu.VMEM((nrows // 2, 1, cols), jnp.float32),
            pltpu.VMEM((8, LANES), jnp.float32),
            pltpu.VMEM((nrows, 8, LANES), jnp.float32),
            pltpu.VMEM((nwidth, 4 * nrows, LANES), jnp.float32),
            pltpu.VMEM((lines, LANES), jnp.float32),
            pltpu.SemaphoreType.REGULAR((2, far - 1)),
            dma((3,)),
            dma((rows // LOAD,)),
            dma(()),
            dma((2, 2)),
            dma(()),
            dma(()),
            dma(()),
            dma(()),
            dma(()),
            dma(()),
            dma(()),
            dma(()),
            dma(()),
            dma(()),
            dma(()),
            dma((2, EARLY)),
            dma(()),
            dma((far * nchunk - EARLY,)),
            dma(()),
            dma(()),
        ],
        compiler_params=pltpu.CompilerParams(
            collective_id=0, has_side_effects=True, vmem_limit_bytes=24 * 1024 * 1024),
        name="gather",
    )(*(pltpu.with_memory_space_constraint(x, pltpu.HBM) for x in (
        one_q, other_q, one_k, other_k, one_v, other_v,
        mix.reshape(1, -1), norm_t.reshape(1, -1), norm_s.reshape(1, -1))))
    q, k, v, scale_q, scale_k, scale_v, norm_o = pl.pallas_call(
        functools.partial(write_kernel, (qd, kd)),
        out_shape=(
            jax.ShapeDtypeStruct((total, qd), jnp.bfloat16),
            jax.ShapeDtypeStruct((total, kd), jnp.bfloat16),
            jax.ShapeDtypeStruct((total, kd), jnp.bfloat16),
            jax.ShapeDtypeStruct((qd // LANES, LANES), jnp.float32),
            jax.ShapeDtypeStruct((1, kd), jnp.float32),
            jax.ShapeDtypeStruct((1, kd), jnp.float32),
            jax.ShapeDtypeStruct((lines, LANES), jnp.bfloat16),
        ),
        in_specs=[vmem] * 5,
        out_specs=(hbm,) * 7,
        scratch_shapes=[dma((10,))],
        compiler_params=pltpu.CompilerParams(vmem_limit_bytes=1024 * 1024),
        name="write",
    )(full, scale_q, scale_k, scale_v, norm)
    return (q, k, v, scale_q.reshape(-1), scale_k.reshape(-1), scale_v.reshape(-1),
            norm_o.reshape(-1))


def solution(mesh):
    rows = ("site", "rows")
    return jax.shard_map(
        functools.partial(shards, mesh.shape["rows"], mesh.shape["width"]),
        mesh=mesh,
        in_specs=(P(rows, "width"),) * 6 + (P(rows), P(("site", "rows", "width")), P(("site", "rows", "width"))),
        out_specs=(P("site", "width"),) * 3 + (P(("site", "width")),) * 3 + (P("site"),),
        check_vma=False,
    )
```

```python
import functools

import jax
import jax.numpy as jnp
from jax import lax
from jax.experimental import pallas as pl
from jax.experimental.pallas import tpu as pltpu
from jax.sharding import PartitionSpec as P

MESH = pl.DeviceIdType.MESH
LANES = 128
LOAD = 64
EARLY = 4
CUTS = (64, 112, 192)
TINY = 1e-30


def bounds_of(rows):
    half = rows // 2
    cuts = [0, *CUTS, half]
    cuts += [half + at for at in cuts[1:]]
    return list(zip(cuts, cuts[1:]))


def gather_kernel(nrows, nwidth, dims, *refs):
    (one_q, other_q, one_k, other_k, one_v, other_v, mix_hbm, norm_t_hbm, norm_s_hbm,
     out, scale_q, scale_k, scale_v, norm_out,
     mix, norm_t, norm_s, a_buf, b_buf, early, mixb, acc, firsts, pair, maxima, seg, tiles, gains, joined,
     tokens, lead_sem, in_sem, sent, first_recv, pair_recv, max_recv, tile_recv, gain_recv, norm_recv, early_recv, ring_recv,
     share_recv) = refs
    rows, qd, kd = dims
    cols = qd + 2 * kd
    nz = nrows // 2
    far = nz // 2
    r = lax.axis_index("rows")
    w = lax.axis_index("width")
    z, c = r // 2, lax.rem(r, 2)
    bounds = bounds_of(rows)
    nchunk = len(bounds)
    root = nrows // 2 + 1
    is_root = r == root

    def row_peer(i):
        return {"rows": lax.rem(r + i, nrows)}

    def width_peer(i):
        return {"width": lax.rem(w + i, nwidth)}

    ahead = (row_peer(2), row_peer(nrows - 2))
    partner = {"rows": r + 1 - 2 * c}
    farthest_first = sorted(range(1, nz), key=lambda i: -min(i, nz - i))

    barrier = pltpu.get_barrier_semaphore()
    for dz in (1, nz - 1):
        for core in (0, 1):
            pl.semaphore_signal(
                barrier, inc=1, device_id={"rows": lax.rem(z + dz, nz) * 2 + core}, device_id_type=MESH)
    pl.semaphore_signal(barrier, inc=1, device_id=partner, device_id_type=MESH)

    @pl.when(is_root)
    def _():
        for i in range(1, nwidth):
            pl.semaphore_signal(barrier, inc=1, device_id=width_peer(i), device_id_type=MESH)

    leads = [
        pltpu.make_async_copy(src, dst, lead_sem.at[i])
        for i, (src, dst) in enumerate(((mix_hbm, mix), (norm_t_hbm, norm_t), (norm_s_hbm, norm_s)))
    ]
    for copy in leads:
        copy.start(priority=1)
    parts = (
        (one_q, a_buf, 0, qd), (other_q, b_buf, 0, qd),
        (one_k, a_buf, qd, kd), (other_k, b_buf, qd, kd),
        (one_v, a_buf, qd + kd, kd), (other_v, b_buf, qd + kd, kd),
    )

    def loads(step):
        span = pl.ds(step * LOAD, LOAD)
        return [
            pltpu.make_async_copy(src.at[span, :], dst.at[span, pl.ds(at, n)], in_sem.at[min(step, 1)])
            for src, dst, at, n in parts
        ]

    def wait_loads(count):
        both = out.at[pl.ds(0, 4 * count), :]
        pltpu.make_async_copy(both, both, in_sem.at[0 if count == LOAD else 1]).wait()

    def spread(at):
        n = min(LANES, rows - at)
        line = mix[:, at:at + n]
        if n < LANES:
            line = jnp.concatenate([line, jnp.zeros((1, LANES - n), jnp.float32)], axis=1)
        square = jnp.transpose(jnp.broadcast_to(line, (LANES, LANES)))
        mixb[at:at + n, :] = square[:n, :]

    def mixed(step):
        span = slice(step * LOAD, (step + 1) * LOAD)
        m = mixb[span, :]
        rest = 1.0 - m
        for at in range(0, cols, LANES):
            lanes = slice(at, at + LANES)
            whole = m * a_buf[span, lanes] + rest * b_buf[span, lanes]
            a_buf[span, lanes] = whole
            top = jnp.max(jnp.abs(whole).reshape(LOAD // 8, 8, LANES), axis=0)
            acc[:, lanes] = top if step == 0 else jnp.maximum(acc[:, lanes], top)

    def coded(chunk, own):
        inverse = 1.0 / jnp.maximum(own, TINY)
        span = slice(*bounds[chunk])
        for at in range(0, cols, LANES):
            lanes = slice(at, at + LANES)
            v = a_buf[span, lanes] * inverse[:, lanes]
            v2 = v * v
            v4 = v2 * v2
            v8 = v4 * v4 * 2.0**63
            code = v8 * v8
            early[2, span, lanes] = jnp.where(v < 0.0, -code, code).astype(early.dtype)

    def early_copy(direction, chunk):
        span = pl.ds(bounds[chunk][0], bounds[chunk][1] - bounds[chunk][0])
        return pltpu.make_async_remote_copy(
            src_ref=early.at[2, span, :], dst_ref=early.at[direction, span, :], send_sem=sent,
            recv_sem=early_recv.at[chunk], device_id=ahead[direction], device_id_type=MESH)

    def first_copy(direction, part):
        return pltpu.make_async_remote_copy(
            src_ref=firsts.at[2, part], dst_ref=firsts.at[direction, part], send_sem=sent,
            recv_sem=first_recv.at[part], device_id=ahead[direction], device_id_type=MESH)

    for copy in loads(0):
        copy.start()
    for copy in leads:
        copy.wait()
    wait_loads(LOAD)
    for step in range(1, rows // LOAD):
        for copy in loads(step):
            copy.start()
    spread(0)
    mixed(0)
    firsts[2, 0] = jnp.max(acc[...], axis=0, keepdims=True)
    coded(0, firsts[2, 0])

    pl.semaphore_wait(barrier, 5 + jnp.where(is_root, nwidth - 1, 0))
    for direction in (0, 1):
        early_copy(direction, 0).start()

    def tell(direction, hop):
        pl.semaphore_signal(tokens.at[direction, hop - 2], inc=1, device_id=ahead[direction], device_id_type=MESH)

    def heard(hop):
        for direction in (0, 1) if hop < far else (0,):
            pl.semaphore_wait(tokens.at[direction, hop - 2], 1)
            if hop + 1 < far or (hop < far and direction == 0):
                tell(direction, hop + 1)

    for direction in (0, 1) if far > 2 else (0,):
        tell(direction, 2)
    for direction in (0, 1):
        first_copy(direction, 0).start()
    heard(2)

    for at in range(LANES, rows, LANES):
        spread(at)
    wait_loads(rows - LOAD)
    for step in range(1, rows // LOAD):
        mixed(step)

    def pair_copy(core):
        return pltpu.make_async_remote_copy(
            src_ref=pair.at[core], dst_ref=pair.at[core], send_sem=sent, recv_sem=pair_recv,
            device_id=partner, device_id_type=MESH)

    firsts[2, 1] = jnp.max(acc[...], axis=0, keepdims=True)
    pair[c] = firsts[2, 1]
    pair_copy(c).start()
    coded(1, firsts[2, 1])
    for direction in (0, 1):
        first_copy(direction, 1).start()
        early_copy(direction, 1).start()
    for hop in range(3, far + 1):
        heard(hop)
    pair_copy(1 - c).wait_recv()
    maxima[z] = jnp.maximum(pair[0], pair[1])

    def max_copy(i):
        return pltpu.make_async_remote_copy(
            src_ref=maxima.at[z], dst_ref=maxima.at[z], send_sem=sent, recv_sem=max_recv,
            device_id=row_peer(2 * i), device_id_type=MESH)

    def all_of(ref, count, send_sem, recv_sem):
        part = ref.at[pl.ds(0, count)]
        return pltpu.make_async_remote_copy(
            src_ref=part, dst_ref=part, send_sem=send_sem, recv_sem=recv_sem, device_id=partner, device_id_type=MESH)

    for i in farthest_first:
        max_copy(i).start()
    for chunk in range(2, EARLY):
        coded(chunk, firsts[2, 1])
        for direction in (0, 1):
            early_copy(direction, chunk).start()

    small = norm_t.shape[1]
    pos = lax.rem(r, 2) * nwidth + w
    first, lane0 = (pos * small) // LANES, lax.rem(pos * small, LANES)
    seg[...] = jnp.zeros((8, LANES), jnp.float32)
    seg[0:1, 0:small] = norm_t[...] + norm_s[...]
    turned = pltpu.roll(seg[...], lane0, 1)[0:1, :]
    lane = lax.broadcasted_iota(jnp.int32, (8, LANES), 1)
    line = lax.broadcasted_iota(jnp.int32, (8, LANES), 0)
    here = ((line == first) & (lane >= lane0)) | ((line == first + 1) & (lane < lane0))
    tiles[r] = jnp.where(here, jnp.broadcast_to(turned, (8, LANES)), 0.0)

    def tile_copy(source):
        return pltpu.make_async_remote_copy(
            src_ref=tiles.at[source], dst_ref=tiles.at[source], send_sem=sent, recv_sem=tile_recv,
            device_id={"rows": root}, device_id_type=MESH)

    def gain_copy(i):
        return pltpu.make_async_remote_copy(
            src_ref=gains.at[w], dst_ref=gains.at[w], send_sem=sent, recv_sem=gain_recv,
            device_id=width_peer(i), device_id_type=MESH)

    def norm_copy(i):
        return pltpu.make_async_remote_copy(
            src_ref=norm_out, dst_ref=norm_out, send_sem=sent, recv_sem=norm_recv,
            device_id=row_peer(i), device_id_type=MESH)

    @pl.when(jnp.logical_not(is_root))
    def _():
        tile_copy(r).start()

    all_of(maxima, nz - 1, sent, max_recv).wait_recv()
    scale = maxima[0]
    for i in range(1, nz):
        scale = jnp.maximum(scale, maxima[i])

    def place(direction, hop, chunk):
        lo, hi = bounds[chunk]
        owner = lax.rem(z - hop + nz, nz) if direction == 0 else lax.rem(z + hop, nz)
        return pl.ds(pl.multiple_of((owner * 2 + c) * rows + lo, 16), hi - lo)

    def landing(hop, chunk):
        return hop * nchunk + chunk - EARLY

    def ring(direction, hop, chunk):
        ref = out.at[place(direction, hop, chunk), :]
        return pltpu.make_async_remote_copy(
            src_ref=ref, dst_ref=ref, send_sem=sent, recv_sem=ring_recv.at[landing(hop, chunk)],
            device_id=ahead[direction], device_id_type=MESH)

    def arrived(hop, chunk):
        lo, hi = bounds[chunk]
        sides = 2 if hop < far else 1
        all_of(out, sides * (hi - lo), sent, ring_recv.at[landing(hop - 1, chunk)]).wait_recv()

    def share(direction, hop, chunk):
        ref = out.at[place(direction, hop, chunk), :]
        return pltpu.make_async_remote_copy(
            src_ref=ref, dst_ref=ref, send_sem=sent, recv_sem=share_recv,
            device_id=partner, device_id_type=MESH)

    def chunks(direction, hop):
        if hop < far:
            return list(range(nchunk))
        return list(range(nchunk // 2)) if direction == 0 else list(range(nchunk // 2, nchunk))

    def rounded(source, direction, hop, chunk):
        at_rows = place(direction, hop, chunk)
        for at in range(0, cols, LANES):
            lanes = slice(at, at + LANES)
            out[at_rows, lanes] = (source[:, lanes] / scale[:, lanes]).astype(out.dtype)

    def decoded(direction, chunk):
        part = min(chunk, 1)
        factor = jnp.maximum(firsts[direction, part], TINY) / scale
        at_rows = place(direction, 1, chunk)
        for at in range(0, cols, LANES):
            lanes = slice(at, at + LANES)
            code = early[direction, bounds[chunk][0]:bounds[chunk][1], lanes].astype(jnp.float32)
            size = jnp.exp2(jnp.log2(jnp.abs(code)) * (1.0 / 16.0) - 126.0 / 16.0)
            out[at_rows, lanes] = (jnp.where(code < 0.0, -size, size) * factor[:, lanes]).astype(out.dtype)

    for chunk in (*range(EARLY, nchunk), *range(EARLY)):
        lo, hi = bounds[chunk]
        rounded(a_buf.at[lo:hi, :], 0, 0, chunk)
        if chunk >= EARLY:
            for direction in (0, 1):
                ring(direction, 0, chunk).start()
        share(0, 0, chunk).start()
    for line in range(qd // LANES):
        scale_q[line:line + 1, :] = scale[:, line * LANES:(line + 1) * LANES]
    scale_k[...] = scale[:, qd:qd + kd]
    scale_v[...] = scale[:, qd + kd:]

    moved = nchunk // 2 - 1

    for hop in range(1, far + 1):
        for step in zip(*(chunks(d, hop) for d in (0, 1))):
            for direction, chunk in enumerate(step):
                if hop == far or (direction == 0 and (hop > 1 or chunk >= EARLY)):
                    arrived(hop, chunk)
                if hop == 1 and chunk < EARLY:
                    if direction == 0:
                        lo, hi = bounds[chunk]
                        if chunk < 2:
                            all_of(pair, 2, sent, first_recv.at[chunk]).wait_recv()
                        all_of(out, 2 * (hi - lo), sent, early_recv.at[chunk]).wait_recv()
                    decoded(direction, chunk)
                if hop + 1 == far and chunk == moved:
                    @pl.when((z != nz - 1) if direction == 0 else (z == 1))
                    def _():
                        ring(direction, hop, chunk).start()
                elif hop + 1 <= far and chunk in chunks(direction, hop + 1):
                    ring(direction, hop, chunk).start()
                share(direction, hop, chunk).start()

        if hop == 1:
            @pl.when(is_root)
            def _():
                all_of(tiles, nrows - 1, sent, tile_recv).wait_recv()
                for g in range(nrows // 2):
                    gains[w, 8 * g:8 * g + 8, :] = tiles[2 * g] + tiles[2 * g + 1]
                for i in range(1, nwidth):
                    gain_copy(i).start()
        if hop == 2:
            @pl.when(is_root)
            def _():
                all_of(gains, nwidth - 1, sent, gain_recv).wait_recv()
                per = 2 * nwidth * small // LANES
                for g in range(nrows // 2):
                    full = gains[0, 8 * g:8 * g + 8, :]
                    for i in range(1, nwidth):
                        full = full + gains[i, 8 * g:8 * g + 8, :]
                    joined[g * per:(g + 1) * per, :] = full[:per, :]
                norm_out[...] = joined[...].astype(norm_out.dtype)
                for i in range(1, nrows):
                    norm_copy(i).start()

    all_of(out, nz * rows, sent, share_recv).wait_recv()
    all_of(out, nz * rows, sent, share_recv).wait_send()
    length = bounds[moved][1] - bounds[moved][0]
    all_of(out, (nz - 1) * rows - 2 * bounds[EARLY - 1][1] - length, sent, ring_recv.at[0]).wait_send()
    for sender in (z != nz - 1, z == 1):
        @pl.when(sender)
        def _():
            all_of(out, length, sent, ring_recv.at[0]).wait_send()
    for direction in (0, 1):
        for part in (0, 1):
            first_copy(direction, part).wait_send()
        for chunk in range(EARLY):
            early_copy(direction, chunk).wait_send()
    pair_copy(c).wait_send()
    all_of(maxima, nz - 1, sent, max_recv).wait_send()

    @pl.when(is_root)
    def _():
        all_of(gains, nwidth - 1, sent, gain_recv).wait_send()
        for i in range(1, nrows):
            norm_copy(i).wait_send()

    @pl.when(jnp.logical_not(is_root))
    def _():
        tile_copy(r).wait_send()
        norm_copy(1).wait_recv()


def write_kernel(dims, full, *refs):
    qd, kd = dims
    q, k, v = refs[4:7]
    sems = refs[-1]
    half = full.shape[0] // 2
    started = []
    for i in range(2):
        span = pl.ds(i * half, half)
        for j, (o, at, n) in enumerate(((q, 0, qd), (k, qd, kd), (v, qd + kd, kd))):
            started.append((i, pltpu.make_async_copy(full.at[span, pl.ds(at, n)], o.at[span, :], sems.at[4 + 3 * i + j])))
    started += [(1, pltpu.make_async_copy(src, dst, sems.at[i])) for i, (src, dst) in enumerate(zip(refs[:4], refs[7:11]))]
    for i, copy in started:
        copy.start(priority=i)
    for i, copy in started:
        copy.wait()


def shards(nrows, nwidth, one_q, other_q, one_k, other_k, one_v, other_v, mix, norm_t, norm_s):
    rows, qd = one_q.shape
    kd = one_k.shape[1]
    cols = qd + 2 * kd
    small = norm_t.shape[0]
    total = rows * nrows
    lines = small * nrows * nwidth // LANES
    far, nchunk = nrows // 4, len(bounds_of(rows))
    early_rows = bounds_of(rows)[EARLY - 1][1]
    dma = pltpu.SemaphoreType.DMA
    hbm = pl.BlockSpec(memory_space=pltpu.HBM)
    vmem = pl.BlockSpec(memory_space=pltpu.VMEM)
    full, scale_q, scale_k, scale_v, norm = pl.pallas_call(
        functools.partial(gather_kernel, nrows, nwidth, (rows, qd, kd)),
        out_shape=(
            pltpu.VMEM((total, cols), jnp.bfloat16),
            pltpu.VMEM((qd // LANES, LANES), jnp.float32),
            pltpu.VMEM((1, kd), jnp.float32),
            pltpu.VMEM((1, kd), jnp.float32),
            pltpu.VMEM((lines, LANES), jnp.bfloat16),
        ),
        in_specs=[hbm] * 9,
        out_specs=(vmem,) * 5,
        scratch_shapes=[
            pltpu.VMEM((1, rows), jnp.float32),
            pltpu.VMEM((1, small), jnp.float32),
            pltpu.VMEM((1, small), jnp.float32),
            pltpu.VMEM((rows, cols), jnp.float32),
            pltpu.VMEM((rows, cols), jnp.float32),
            pltpu.VMEM((3, early_rows, cols), jnp.bfloat16),
            pltpu.VMEM((rows, LANES), jnp.float32),
            pltpu.VMEM((8, cols), jnp.float32),
            pltpu.VMEM((3, 2, 1, cols), jnp.float32),
            pltpu.VMEM((2, 1, cols), jnp.float32),
            pltpu.VMEM((nrows // 2, 1, cols), jnp.float32),
            pltpu.VMEM((8, LANES), jnp.float32),
            pltpu.VMEM((nrows, 8, LANES), jnp.float32),
            pltpu.VMEM((nwidth, 4 * nrows, LANES), jnp.float32),
            pltpu.VMEM((lines, LANES), jnp.float32),
            pltpu.SemaphoreType.REGULAR((2, far - 1)),
            dma((3,)),
            dma((2,)),
            dma(()),
            dma((2,)),
            dma(()),
            dma(()),
            dma(()),
            dma(()),
            dma(()),
            dma((EARLY,)),
            dma((far * nchunk - EARLY,)),
            dma(()),
        ],
        compiler_params=pltpu.CompilerParams(
            collective_id=0, has_side_effects=True, vmem_limit_bytes=24 * 1024 * 1024),
        name="gather",
    )(*(pltpu.with_memory_space_constraint(x, pltpu.HBM) for x in (
        one_q, other_q, one_k, other_k, one_v, other_v,
        mix.reshape(1, -1), norm_t.reshape(1, -1), norm_s.reshape(1, -1))))
    q, k, v, scale_q, scale_k, scale_v, norm_o = pl.pallas_call(
        functools.partial(write_kernel, (qd, kd)),
        out_shape=(
            jax.ShapeDtypeStruct((total, qd), jnp.bfloat16),
            jax.ShapeDtypeStruct((total, kd), jnp.bfloat16),
            jax.ShapeDtypeStruct((total, kd), jnp.bfloat16),
            jax.ShapeDtypeStruct((qd // LANES, LANES), jnp.float32),
            jax.ShapeDtypeStruct((1, kd), jnp.float32),
            jax.ShapeDtypeStruct((1, kd), jnp.float32),
            jax.ShapeDtypeStruct((lines, LANES), jnp.bfloat16),
        ),
        in_specs=[vmem] * 5,
        out_specs=(hbm,) * 7,
        scratch_shapes=[dma((10,))],
        compiler_params=pltpu.CompilerParams(vmem_limit_bytes=1024 * 1024),
        name="write",
    )(full, scale_q, scale_k, scale_v, norm)
    return (q, k, v, scale_q.reshape(-1), scale_k.reshape(-1), scale_v.reshape(-1),
            norm_o.reshape(-1))


def solution(mesh):
    rows = ("site", "rows")
    return jax.shard_map(
        functools.partial(shards, mesh.shape["rows"], mesh.shape["width"]),
        mesh=mesh,
        in_specs=(P(rows, "width"),) * 6 + (P(rows), P(("site", "rows", "width")), P(("site", "rows", "width"))),
        out_specs=(P("site", "width"),) * 3 + (P(("site", "width")),) * 3 + (P("site"),),
        check_vma=False,
    )
```

```python
import functools

import jax
import jax.numpy as jnp
from jax import lax
from jax.experimental import pallas as pl
from jax.experimental.pallas import tpu as pltpu
from jax.sharding import PartitionSpec as P

MESH = pl.DeviceIdType.MESH
LANES = 128
LOAD = 64
EARLY = 4
CUTS = (64, 112, 192)
TINY = 1e-30


def bounds_of(rows):
    half = rows // 2
    cuts = [0, *CUTS, half]
    cuts += [half + at for at in cuts[1:]]
    return list(zip(cuts, cuts[1:]))


def gather_kernel(nrows, nwidth, dims, *refs):
    (one_q, other_q, one_k, other_k, one_v, other_v, mix_hbm, norm_t_hbm, norm_s_hbm,
     out, scale_q, scale_k, scale_v, norm_out,
     mix, norm_t, norm_s, a_buf, b_buf, early, mixb, acc, firsts, pair, maxima, seg, tiles, gains, joined,
     tokens, lead_sem, in_sem, sent, first_recv, pair_recv, max_recv, tile_recv, gain_recv, norm_recv, early_recv, ring_recv,
     share_recv) = refs
    rows, qd, kd = dims
    cols = qd + 2 * kd
    nz = nrows // 2
    far = nz // 2
    r = lax.axis_index("rows")
    w = lax.axis_index("width")
    z, c = r // 2, lax.rem(r, 2)
    bounds = bounds_of(rows)
    nchunk = len(bounds)
    root = nrows // 2 + 1
    is_root = r == root

    def row_peer(i):
        return {"rows": lax.rem(r + i, nrows)}

    def width_peer(i):
        return {"width": lax.rem(w + i, nwidth)}

    ahead = (row_peer(2), row_peer(nrows - 2))
    partner = {"rows": r + 1 - 2 * c}
    farthest_first = sorted(range(1, nz), key=lambda i: -min(i, nz - i))

    barrier = pltpu.get_barrier_semaphore()
    for dz in (1, nz - 1):
        for core in (0, 1):
            pl.semaphore_signal(
                barrier, inc=1, device_id={"rows": lax.rem(z + dz, nz) * 2 + core}, device_id_type=MESH)
    pl.semaphore_signal(barrier, inc=1, device_id=partner, device_id_type=MESH)

    @pl.when(is_root)
    def _():
        for i in range(1, nwidth):
            pl.semaphore_signal(barrier, inc=1, device_id=width_peer(i), device_id_type=MESH)

    leads = [
        pltpu.make_async_copy(src, dst, lead_sem.at[i])
        for i, (src, dst) in enumerate(((mix_hbm, mix), (norm_t_hbm, norm_t), (norm_s_hbm, norm_s)))
    ]
    for copy in leads:
        copy.start(priority=1)
    parts = (
        (one_q, a_buf, 0, qd), (other_q, b_buf, 0, qd),
        (one_k, a_buf, qd, kd), (other_k, b_buf, qd, kd),
        (one_v, a_buf, qd + kd, kd), (other_v, b_buf, qd + kd, kd),
    )

    def loads(step):
        span = pl.ds(step * LOAD, LOAD)
        return [
            pltpu.make_async_copy(src.at[span, :], dst.at[span, pl.ds(at, n)], in_sem.at[min(step, 1)])
            for src, dst, at, n in parts
        ]

    def wait_loads(count):
        both = out.at[pl.ds(0, 4 * count), :]
        pltpu.make_async_copy(both, both, in_sem.at[0 if count == LOAD else 1]).wait()

    def spread(at):
        n = min(LANES, rows - at)
        line = mix[:, at:at + n]
        if n < LANES:
            line = jnp.concatenate([line, jnp.zeros((1, LANES - n), jnp.float32)], axis=1)
        square = jnp.transpose(jnp.broadcast_to(line, (LANES, LANES)))
        mixb[at:at + n, :] = square[:n, :]

    def mixed(step):
        span = slice(step * LOAD, (step + 1) * LOAD)
        m = mixb[span, :]
        rest = 1.0 - m
        for at in range(0, cols, LANES):
            lanes = slice(at, at + LANES)
            whole = m * a_buf[span, lanes] + rest * b_buf[span, lanes]
            a_buf[span, lanes] = whole
            top = jnp.max(jnp.abs(whole).reshape(LOAD // 8, 8, LANES), axis=0)
            acc[:, lanes] = top if step == 0 else jnp.maximum(acc[:, lanes], top)

    def coded(chunk, own):
        inverse = 1.0 / jnp.maximum(own, TINY)
        span = slice(*bounds[chunk])
        for at in range(0, cols, LANES):
            lanes = slice(at, at + LANES)
            v = a_buf[span, lanes] * inverse[:, lanes]
            v2 = v * v
            v4 = v2 * v2
            v8 = v4 * v4 * 2.0**63
            code = v8 * v8
            early[2, span, lanes] = jnp.where(v < 0.0, -code, code).astype(early.dtype)

    def early_copy(direction, chunk):
        span = pl.ds(bounds[chunk][0], bounds[chunk][1] - bounds[chunk][0])
        return pltpu.make_async_remote_copy(
            src_ref=early.at[2, span, :], dst_ref=early.at[direction, span, :], send_sem=sent,
            recv_sem=early_recv.at[chunk], device_id=ahead[direction], device_id_type=MESH)

    def first_copy(direction, part):
        return pltpu.make_async_remote_copy(
            src_ref=firsts.at[2, part], dst_ref=firsts.at[direction, part], send_sem=sent,
            recv_sem=first_recv.at[part], device_id=ahead[direction], device_id_type=MESH)

    for copy in loads(0):
        copy.start()
    for copy in leads:
        copy.wait()
    wait_loads(LOAD)
    for step in range(1, rows // LOAD):
        for copy in loads(step):
            copy.start()
    spread(0)
    mixed(0)
    firsts[2, 0] = jnp.max(acc[...], axis=0, keepdims=True)
    coded(0, firsts[2, 0])

    pl.semaphore_wait(barrier, 5 + jnp.where(is_root, nwidth - 1, 0))
    for direction in (0, 1):
        early_copy(direction, 0).start()

    def tell(direction, hop):
        pl.semaphore_signal(tokens.at[direction, hop - 2], inc=1, device_id=ahead[direction], device_id_type=MESH)

    def heard(hop):
        for direction in (0, 1) if hop < far else (0,):
            pl.semaphore_wait(tokens.at[direction, hop - 2], 1)
            if hop + 1 < far or (hop < far and direction == 0):
                tell(direction, hop + 1)

    for direction in (0, 1) if far > 2 else (0,):
        tell(direction, 2)
    for direction in (0, 1):
        first_copy(direction, 0).start()
    heard(2)

    for at in range(LANES, rows, LANES):
        spread(at)
    wait_loads(rows - LOAD)
    for step in range(1, rows // LOAD):
        mixed(step)

    def pair_copy(core):
        return pltpu.make_async_remote_copy(
            src_ref=pair.at[core], dst_ref=pair.at[core], send_sem=sent, recv_sem=pair_recv,
            device_id=partner, device_id_type=MESH)

    firsts[2, 1] = jnp.max(acc[...], axis=0, keepdims=True)
    pair[c] = firsts[2, 1]
    pair_copy(c).start()
    coded(1, firsts[2, 1])
    for direction in (0, 1):
        first_copy(direction, 1).start()
        early_copy(direction, 1).start()
    for hop in range(3, far + 1):
        heard(hop)
    pair_copy(1 - c).wait_recv()
    maxima[z] = jnp.maximum(pair[0], pair[1])

    def max_copy(i):
        return pltpu.make_async_remote_copy(
            src_ref=maxima.at[z], dst_ref=maxima.at[z], send_sem=sent, recv_sem=max_recv,
            device_id=row_peer(2 * i), device_id_type=MESH)

    def all_of(ref, count, send_sem, recv_sem):
        part = ref.at[pl.ds(0, count)]
        return pltpu.make_async_remote_copy(
            src_ref=part, dst_ref=part, send_sem=send_sem, recv_sem=recv_sem, device_id=partner, device_id_type=MESH)

    for i in farthest_first:
        max_copy(i).start()
    for chunk in range(2, EARLY):
        coded(chunk, firsts[2, 1])
        for direction in (0, 1):
            early_copy(direction, chunk).start()

    small = norm_t.shape[1]
    pos = lax.rem(r, 2) * nwidth + w
    first, lane0 = (pos * small) // LANES, lax.rem(pos * small, LANES)
    seg[...] = jnp.zeros((8, LANES), jnp.float32)
    seg[0:1, 0:small] = norm_t[...] + norm_s[...]
    turned = pltpu.roll(seg[...], lane0, 1)[0:1, :]
    lane = lax.broadcasted_iota(jnp.int32, (8, LANES), 1)
    line = lax.broadcasted_iota(jnp.int32, (8, LANES), 0)
    here = ((line == first) & (lane >= lane0)) | ((line == first + 1) & (lane < lane0))
    tiles[r] = jnp.where(here, jnp.broadcast_to(turned, (8, LANES)), 0.0)

    def tile_copy(source):
        return pltpu.make_async_remote_copy(
            src_ref=tiles.at[source], dst_ref=tiles.at[source], send_sem=sent, recv_sem=tile_recv,
            device_id={"rows": root}, device_id_type=MESH)

    def gain_copy(i):
        return pltpu.make_async_remote_copy(
            src_ref=gains.at[w], dst_ref=gains.at[w], send_sem=sent, recv_sem=gain_recv,
            device_id=width_peer(i), device_id_type=MESH)

    def norm_copy(i):
        return pltpu.make_async_remote_copy(
            src_ref=norm_out, dst_ref=norm_out, send_sem=sent, recv_sem=norm_recv,
            device_id=row_peer(i), device_id_type=MESH)

    @pl.when(jnp.logical_not(is_root))
    def _():
        tile_copy(r).start()

    all_of(maxima, nz - 1, sent, max_recv).wait_recv()
    scale = maxima[0]
    for i in range(1, nz):
        scale = jnp.maximum(scale, maxima[i])

    def place(direction, hop, chunk):
        lo, hi = bounds[chunk]
        owner = lax.rem(z - hop + nz, nz) if direction == 0 else lax.rem(z + hop, nz)
        return pl.ds(pl.multiple_of((owner * 2 + c) * rows + lo, 16), hi - lo)

    def landing(hop, chunk):
        return hop * nchunk + chunk - EARLY

    def ring(direction, hop, chunk):
        ref = out.at[place(direction, hop, chunk), :]
        return pltpu.make_async_remote_copy(
            src_ref=ref, dst_ref=ref, send_sem=sent, recv_sem=ring_recv.at[landing(hop, chunk)],
            device_id=ahead[direction], device_id_type=MESH)

    def arrived(hop, chunk):
        lo, hi = bounds[chunk]
        sides = 2 if hop < far else 1
        all_of(out, sides * (hi - lo), sent, ring_recv.at[landing(hop - 1, chunk)]).wait_recv()

    def share(direction, hop, chunk):
        ref = out.at[place(direction, hop, chunk), :]
        return pltpu.make_async_remote_copy(
            src_ref=ref, dst_ref=ref, send_sem=sent, recv_sem=share_recv,
            device_id=partner, device_id_type=MESH)

    def chunks(direction, hop):
        if hop < far:
            return list(range(nchunk))
        return list(range(nchunk // 2)) if direction == 0 else list(range(nchunk // 2, nchunk))

    def rounded(source, direction, hop, chunk):
        at_rows = place(direction, hop, chunk)
        for at in range(0, cols, LANES):
            lanes = slice(at, at + LANES)
            out[at_rows, lanes] = (source[:, lanes] / scale[:, lanes]).astype(out.dtype)

    def decoded(direction, hop, chunk):
        slot = direction if hop else 2
        part = min(chunk, 1)
        factor = jnp.maximum(firsts[slot, part], TINY) / scale
        at_rows = place(direction, hop, chunk)
        for at in range(0, cols, LANES):
            lanes = slice(at, at + LANES)
            code = early[slot, bounds[chunk][0]:bounds[chunk][1], lanes].astype(jnp.float32)
            size = jnp.exp2(jnp.log2(jnp.abs(code)) * (1.0 / 16.0) - 126.0 / 16.0)
            out[at_rows, lanes] = (jnp.where(code < 0.0, -size, size) * factor[:, lanes]).astype(out.dtype)

    for chunk in (*range(EARLY, nchunk), *range(EARLY)):
        if chunk < EARLY:
            decoded(0, 0, chunk)
        else:
            lo, hi = bounds[chunk]
            rounded(a_buf.at[lo:hi, :], 0, 0, chunk)
            for direction in (0, 1):
                ring(direction, 0, chunk).start()
        share(0, 0, chunk).start()
    for line in range(qd // LANES):
        scale_q[line:line + 1, :] = scale[:, line * LANES:(line + 1) * LANES]
    scale_k[...] = scale[:, qd:qd + kd]
    scale_v[...] = scale[:, qd + kd:]

    moved = nchunk // 2 - 1

    for hop in range(1, far + 1):
        for step in zip(*(chunks(d, hop) for d in (0, 1))):
            for direction, chunk in enumerate(step):
                if hop == far or (direction == 0 and (hop > 1 or chunk >= EARLY)):
                    arrived(hop, chunk)
                if hop == 1 and chunk < EARLY:
                    if direction == 0:
                        lo, hi = bounds[chunk]
                        if chunk < 2:
                            all_of(pair, 2, sent, first_recv.at[chunk]).wait_recv()
                        all_of(out, 2 * (hi - lo), sent, early_recv.at[chunk]).wait_recv()
                    decoded(direction, hop, chunk)
                if hop + 1 == far and chunk == moved:
                    @pl.when((z != nz - 1) if direction == 0 else (z == 1))
                    def _():
                        ring(direction, hop, chunk).start()
                elif hop + 1 <= far and chunk in chunks(direction, hop + 1):
                    ring(direction, hop, chunk).start()
                share(direction, hop, chunk).start()

        if hop == 1:
            @pl.when(is_root)
            def _():
                all_of(tiles, nrows - 1, sent, tile_recv).wait_recv()
                for g in range(nrows // 2):
                    gains[w, 8 * g:8 * g + 8, :] = tiles[2 * g] + tiles[2 * g + 1]
                for i in range(1, nwidth):
                    gain_copy(i).start()
        if hop == 2:
            @pl.when(is_root)
            def _():
                all_of(gains, nwidth - 1, sent, gain_recv).wait_recv()
                per = 2 * nwidth * small // LANES
                for g in range(nrows // 2):
                    full = gains[0, 8 * g:8 * g + 8, :]
                    for i in range(1, nwidth):
                        full = full + gains[i, 8 * g:8 * g + 8, :]
                    joined[g * per:(g + 1) * per, :] = full[:per, :]
                norm_out[...] = joined[...].astype(norm_out.dtype)
                for i in range(1, nrows):
                    norm_copy(i).start()

    all_of(out, nz * rows, sent, share_recv).wait_recv()
    all_of(out, nz * rows, sent, share_recv).wait_send()
    length = bounds[moved][1] - bounds[moved][0]
    all_of(out, (nz - 1) * rows - 2 * bounds[EARLY - 1][1] - length, sent, ring_recv.at[0]).wait_send()
    for sender in (z != nz - 1, z == 1):
        @pl.when(sender)
        def _():
            all_of(out, length, sent, ring_recv.at[0]).wait_send()
    for direction in (0, 1):
        for part in (0, 1):
            first_copy(direction, part).wait_send()
        for chunk in range(EARLY):
            early_copy(direction, chunk).wait_send()
    pair_copy(c).wait_send()
    all_of(maxima, nz - 1, sent, max_recv).wait_send()

    @pl.when(is_root)
    def _():
        all_of(gains, nwidth - 1, sent, gain_recv).wait_send()
        for i in range(1, nrows):
            norm_copy(i).wait_send()

    @pl.when(jnp.logical_not(is_root))
    def _():
        tile_copy(r).wait_send()
        norm_copy(1).wait_recv()


def write_kernel(dims, full, *refs):
    qd, kd = dims
    q, k, v = refs[4:7]
    sems = refs[-1]
    half = full.shape[0] // 2
    started = []
    for i in range(2):
        span = pl.ds(i * half, half)
        for j, (o, at, n) in enumerate(((q, 0, qd), (k, qd, kd), (v, qd + kd, kd))):
            started.append((i, pltpu.make_async_copy(full.at[span, pl.ds(at, n)], o.at[span, :], sems.at[4 + 3 * i + j])))
    started += [(1, pltpu.make_async_copy(src, dst, sems.at[i])) for i, (src, dst) in enumerate(zip(refs[:4], refs[7:11]))]
    for i, copy in started:
        copy.start(priority=i)
    for i, copy in started:
        copy.wait()


def shards(nrows, nwidth, one_q, other_q, one_k, other_k, one_v, other_v, mix, norm_t, norm_s):
    rows, qd = one_q.shape
    kd = one_k.shape[1]
    cols = qd + 2 * kd
    small = norm_t.shape[0]
    total = rows * nrows
    lines = small * nrows * nwidth // LANES
    far, nchunk = nrows // 4, len(bounds_of(rows))
    early_rows = bounds_of(rows)[EARLY - 1][1]
    dma = pltpu.SemaphoreType.DMA
    hbm = pl.BlockSpec(memory_space=pltpu.HBM)
    vmem = pl.BlockSpec(memory_space=pltpu.VMEM)
    full, scale_q, scale_k, scale_v, norm = pl.pallas_call(
        functools.partial(gather_kernel, nrows, nwidth, (rows, qd, kd)),
        out_shape=(
            pltpu.VMEM((total, cols), jnp.bfloat16),
            pltpu.VMEM((qd // LANES, LANES), jnp.float32),
            pltpu.VMEM((1, kd), jnp.float32),
            pltpu.VMEM((1, kd), jnp.float32),
            pltpu.VMEM((lines, LANES), jnp.bfloat16),
        ),
        in_specs=[hbm] * 9,
        out_specs=(vmem,) * 5,
        scratch_shapes=[
            pltpu.VMEM((1, rows), jnp.float32),
            pltpu.VMEM((1, small), jnp.float32),
            pltpu.VMEM((1, small), jnp.float32),
            pltpu.VMEM((rows, cols), jnp.float32),
            pltpu.VMEM((rows, cols), jnp.float32),
            pltpu.VMEM((3, early_rows, cols), jnp.bfloat16),
            pltpu.VMEM((rows, LANES), jnp.float32),
            pltpu.VMEM((8, cols), jnp.float32),
            pltpu.VMEM((3, 2, 1, cols), jnp.float32),
            pltpu.VMEM((2, 1, cols), jnp.float32),
            pltpu.VMEM((nrows // 2, 1, cols), jnp.float32),
            pltpu.VMEM((8, LANES), jnp.float32),
            pltpu.VMEM((nrows, 8, LANES), jnp.float32),
            pltpu.VMEM((nwidth, 4 * nrows, LANES), jnp.float32),
            pltpu.VMEM((lines, LANES), jnp.float32),
            pltpu.SemaphoreType.REGULAR((2, far - 1)),
            dma((3,)),
            dma((2,)),
            dma(()),
            dma((2,)),
            dma(()),
            dma(()),
            dma(()),
            dma(()),
            dma(()),
            dma((EARLY,)),
            dma((far * nchunk - EARLY,)),
            dma(()),
        ],
        compiler_params=pltpu.CompilerParams(
            collective_id=0, has_side_effects=True, vmem_limit_bytes=24 * 1024 * 1024),
        name="gather",
    )(*(pltpu.with_memory_space_constraint(x, pltpu.HBM) for x in (
        one_q, other_q, one_k, other_k, one_v, other_v,
        mix.reshape(1, -1), norm_t.reshape(1, -1), norm_s.reshape(1, -1))))
    q, k, v, scale_q, scale_k, scale_v, norm_o = pl.pallas_call(
        functools.partial(write_kernel, (qd, kd)),
        out_shape=(
            jax.ShapeDtypeStruct((total, qd), jnp.bfloat16),
            jax.ShapeDtypeStruct((total, kd), jnp.bfloat16),
            jax.ShapeDtypeStruct((total, kd), jnp.bfloat16),
            jax.ShapeDtypeStruct((qd // LANES, LANES), jnp.float32),
            jax.ShapeDtypeStruct((1, kd), jnp.float32),
            jax.ShapeDtypeStruct((1, kd), jnp.float32),
            jax.ShapeDtypeStruct((lines, LANES), jnp.bfloat16),
        ),
        in_specs=[vmem] * 5,
        out_specs=(hbm,) * 7,
        scratch_shapes=[dma((10,))],
        compiler_params=pltpu.CompilerParams(vmem_limit_bytes=1024 * 1024),
        name="write",
    )(full, scale_q, scale_k, scale_v, norm)
    return (q, k, v, scale_q.reshape(-1), scale_k.reshape(-1), scale_v.reshape(-1),
            norm_o.reshape(-1))


def solution(mesh):
    rows = ("site", "rows")
    return jax.shard_map(
        functools.partial(shards, mesh.shape["rows"], mesh.shape["width"]),
        mesh=mesh,
        in_specs=(P(rows, "width"),) * 6 + (P(rows), P(("site", "rows", "width")), P(("site", "rows", "width"))),
        out_specs=(P("site", "width"),) * 3 + (P(("site", "width")),) * 3 + (P("site"),),
        check_vma=False,
    )
```
